32 devices in a mesh: dp: 1, tp: 32 (over x, y, z, core).
Axes of the slice: x: 2, y: 2, z: 4, core: 2. Of those that a mesh axis runs over, the one named last changes fastest.
Arguments:
- x: bfloat16 [2048, 8192], P('dp')
- dy: bfloat16 [2048, 8192], P('dp')
- gate: bfloat16 [2048, 32768], P('dp', 'tp')
- up: bfloat16 [2048, 32768], P('dp', 'tp')
- w_gate: bfloat16 [8192, 32768], P(None, 'tp')
- w_up: bfloat16 [8192, 32768], P(None, 'tp')
- w_down: bfloat16 [32768, 8192], P('tp')
Outputs:
- output 1: bfloat16 [2048, 8192], P('dp')
- output 2: bfloat16 [8192, 32768], P('dp', 'tp')
- output 3: bfloat16 [8192, 32768], P('dp', 'tp')
- output 4: bfloat16 [32768, 8192], P(('dp', 'tp'))
All inputs are finite; a program needn't handle non-finite values.
Results may differ from the reference program's by a relative error of at most 0.012.
Values are sent between devices in bfloat16 or wider.
A program may use at most 2 GiB of HBM per device.

```python
import jax
import jax.numpy as jnp

ROWS = 2048
D = 8192
FF = 32768


def act(gate, up):
    return jax.nn.silu(gate) * up


def setup_inputs(seed: int = 0, part: int = 0) -> dict:
    kx, ky, ka, kb, kg, ku, kd = jax.random.split(jax.random.key(seed), 7)
    kx, ky, ka, kb = (jax.random.fold_in(k, part) for k in (kx, ky, ka, kb))
    drawn = {
        "x": jax.random.normal(kx, (ROWS, D), jnp.float32),
        "dy": jax.random.normal(ky, (ROWS, D), jnp.float32),
        "gate": jax.random.normal(ka, (ROWS, FF), jnp.float32),
        "up": jax.random.normal(kb, (ROWS, FF), jnp.float32),
        "w_gate": jax.random.normal(kg, (D, FF), jnp.float32) * D**-0.5,
        "w_up": jax.random.normal(ku, (D, FF), jnp.float32) * D**-0.5,
        "w_down": jax.random.normal(kd, (FF, D), jnp.float32) * FF**-0.5,
    }
    return {k: v.astype(jnp.bfloat16) for k, v in drawn.items()}


def reference(x, dy, gate, up, w_gate, w_up, w_down):
    hidden, back = jax.vjp(act, gate.astype(jnp.float32), up.astype(jnp.float32))
    d_hidden = jnp.dot(dy, w_down.T, preferred_element_type=jnp.float32)
    d_gate, d_up = (g.astype(jnp.bfloat16) for g in back(d_hidden))
    dx = jnp.dot(d_gate, w_gate.T, preferred_element_type=jnp.float32) + jnp.dot(d_up, w_up.T, preferred_element_type=jnp.float32)
    dw_gate = jnp.dot(x.T, d_gate, preferred_element_type=jnp.float32)
    dw_up = jnp.dot(x.T, d_up, preferred_element_type=jnp.float32)
    dw_down = jnp.dot(hidden.astype(jnp.bfloat16).T, dy, preferred_element_type=jnp.float32)
    return tuple(g.astype(jnp.bfloat16) for g in (dx, dw_gate, dw_up, dw_down))
```

```python
import functools

import jax
import jax.numpy as jnp
from jax import lax
from jax.experimental import pallas as pl
from jax.experimental.pallas import tpu as pltpu
from jax.sharding import PartitionSpec as P

BF, F32 = jnp.bfloat16, jnp.float32
MESH = pl.DeviceIdType.MESH
NT = (((1,), (1,)), ((), ()))
TN = (((0,), (0,)), ((), ()))

QUARTERS = 4
COLS = 8
CHUNKS = QUARTERS * COLS
KBLOCKS = 4
UNITS = 16
DH = QUARTERS * KBLOCKS
E1, E2, E3, E4, E5, E6, E7, E8, E9, E10, E11, E12 = 1, 5, 8, 10, 12, 14, 15, 17, 19, 22, 26, 28
FIRST = KBLOCKS
DW_GROUP = (DH - KBLOCKS) // 2
TICKS = FIRST + max(4 * (DW_GROUP + UNITS), 2 * CHUNKS + E12)


def dot(a, b, dims):
    return lax.dot_general(a, b, dims, preferred_element_type=F32)


def add_rows(dst, a, b, rows, block):
    def body(i, _):
        r = pl.ds(pl.multiple_of(i * block, block), block)
        dst[r] = (a[r].astype(F32) + b[r].astype(F32)).astype(BF)

    lax.fori_loop(0, rows // block, body, None)


def main_kernel(
    x, dy, gate, up, w_gate, w_up, w_down, dx, hid, dw,
    d, w_buf, wd_buf, dy_buf, x_buf, g_buf, u_buf, acc, h_buf, o_buf,
    term, r_d, s1, r_1, s2, z_r, z_l, r_3,
    w_sem, dh_sem, x_sem, gu_sem, h_sem, o_sem, loc_sem,
    d_snd, d_rcv, s1_snd, s1_rcv, zr_snd, zr_rcv, zl_snd, zl_rcv, s3_snd, s3_rcv,
    a3_snd, a3_rcv, gr_snd, gr_rcv, gl_snd, gl_rcv, a1_snd, a1_rcv, ad_snd, ad_rcv,
):
    rows, cols = dy.shape
    ff = gate.shape[1]
    qr, nc, kb, xt = rows // QUARTERS, cols // COLS, cols // KBLOCKS, cols // UNITS
    half, quart, piece, last = qr // 2, qr // 4, qr // 16, qr // 32

    me = lax.axis_index("tp")
    core, z = lax.rem(me, 2), lax.rem(lax.div(me, 2), 4)
    y, xx = lax.rem(lax.div(me, 8), 2), lax.div(me, 16)
    n_d = me + 1 - 2 * core
    n_x, n_y = me + 16 * (1 - 2 * xx), me + 8 * (1 - 2 * y)
    n_r, n_l = me + 2, me - 2

    def copy(src, dst, sem):
        return pltpu.make_async_copy(src, dst, sem)

    def remote(src, dst, snd, rcv, to):
        return pltpu.make_async_remote_copy(
            src_ref=src, dst_ref=dst, send_sem=snd, recv_sem=rcv,
            device_id={"tp": to}, device_id_type=MESH,
        )

    def dh_loads(m):
        q, j, slot = lax.div(m, KBLOCKS), lax.rem(m, KBLOCKS), lax.rem(m, 2)
        k = pl.ds(pl.multiple_of(j * kb, kb), kb)
        r = pl.ds(pl.multiple_of(q * qr, qr), qr)
        return (
            copy(dy.at[r, k], dy_buf.at[slot], dh_sem.at[0, slot]),
            copy(w_down.at[:, k], wd_buf.at[slot], dh_sem.at[1, slot]),
        )

    def gu_loads(q):
        r = pl.ds(pl.multiple_of(q * qr, qr), qr)
        return copy(gate.at[r], g_buf, gu_sem.at[0]), copy(up.at[r], u_buf, gu_sem.at[1])

    def w_loads(k):
        slot = lax.rem(k, 2)
        r = pl.ds(pl.multiple_of(lax.rem(k, COLS) * nc, nc), nc)
        return (
            copy(w_gate.at[r], w_buf.at[slot, :, pl.ds(0, ff)], w_sem.at[0, slot]),
            copy(w_up.at[r], w_buf.at[slot, :, pl.ds(ff, ff)], w_sem.at[1, slot]),
        )

    def x_load(u):
        slot = lax.rem(u, 2)
        return copy(x.at[:, pl.ds(pl.multiple_of(u * xt, xt), xt)], x_buf.at[slot], x_sem.at[slot])

    def o_store(u, j):
        return copy(o_buf.at[j], dw.at[j, pl.ds(pl.multiple_of(u * xt, xt), xt)], o_sem.at[j])

    def h_store(q):
        return copy(h_buf, hid.at[pl.ds(pl.multiple_of(q * qr, qr), qr)], h_sem)

    def go(*copies):
        for c in copies:
            c.start()

    def wait(*copies):
        for c in copies:
            c.wait()

    go(*dh_loads(0))
    go(*dh_loads(1))
    go(*gu_loads(0))
    go(*w_loads(0))
    go(*w_loads(1))

    barrier = pltpu.get_barrier_semaphore()
    for to in (n_d, n_x, n_y):
        pl.semaphore_signal(barrier, inc=1, device_id={"tp": to}, device_id_type=MESH)

    @pl.when(z > 0)
    def _():
        pl.semaphore_signal(barrier, inc=1, device_id={"tp": n_l}, device_id_type=MESH)

    @pl.when(z < 3)
    def _():
        pl.semaphore_signal(barrier, inc=1, device_id={"tp": n_r}, device_id_type=MESH)

    pl.semaphore_wait(barrier, jnp.where((z > 0) & (z < 3), 5, 4))

    def chunk(k):
        q, n, odd = lax.div(k, COLS), lax.rem(k, COLS), lax.rem(k, 2)
        b1, b3 = jnp.where(odd == 0, xx, y), jnp.where(odd == 0, y, xx)
        to1, to3 = jnp.where(odd == 0, n_x, n_y), jnp.where(odd == 0, n_y, n_x)
        return q * qr, n * nc, b1, b3, to1, to3

    def at_out(row, count, col):
        return dx.at[pl.ds(pl.multiple_of(row, last), count), pl.ds(pl.multiple_of(col, nc), nc)]

    def send_d(k):
        s = lax.rem(k, 2)
        src = term.at[s, pl.ds(pl.multiple_of((1 - core) * half, half), half)]
        return remote(src, r_d.at[lax.rem(k, 4)], d_snd.at[s], d_rcv.at[lax.rem(k, 4)], n_d)

    def send_1(k):
        _, _, b1, _, to1, _ = chunk(k)
        src = s1.at[lax.rem(k, 4), pl.ds(pl.multiple_of((1 - b1) * quart, quart), quart)]
        return remote(src, r_1.at[lax.rem(k, 8)], s1_snd.at[lax.rem(k, 4)], s1_rcv.at[lax.rem(k, 8)], to1)

    def send_zr(k, row, count):
        s = lax.rem(k, 8)
        return remote(s2.at[s, pl.ds(row, count)], z_r.at[s, pl.ds(0, count)], zr_snd.at[s], zr_rcv.at[s], n_r)

    def send_zl(k, row, count):
        s = lax.rem(k, 8)
        return remote(s2.at[s, pl.ds(row, count)], z_l.at[s, pl.ds(0, count)], zl_snd.at[s], zl_rcv.at[s], n_l)

    def send_3(k):
        _, _, _, b3, _, to3 = chunk(k)
        src = s2.at[lax.rem(k, 8), pl.ds(pl.multiple_of(z * piece + (1 - b3) * last, last), last)]
        return remote(src, r_3.at[lax.rem(k, 4)], s3_snd.at[lax.rem(k, 4)], s3_rcv.at[lax.rem(k, 4)], to3)

    def final_rows(k):
        row, col, b1, b3, _, _ = chunk(k)
        return (
            s2.at[lax.rem(k, 8), pl.ds(pl.multiple_of(z * piece + b3 * last, last), last)],
            at_out(row + core * half + b1 * quart + z * piece + b3 * last, last, col),
        )

    def keep_final(k):
        src, dst = final_rows(k)
        return copy(src, dst, loc_sem.at[lax.rem(k, 4)])

    def gather_3(k):
        src, dst = final_rows(k)
        s = lax.rem(k, 8)
        return remote(src, dst, a3_snd.at[s], a3_rcv.at[s], chunk(k)[5])

    def gather_r(k, first, count):
        row, col, b1, _, _, _ = chunk(k)
        ref = at_out(row + core * half + b1 * quart + first * piece, count * piece, col)
        s = lax.rem(k, 8)
        return remote(ref, ref, gr_snd.at[s], gr_rcv.at[s], n_r)

    def gather_l(k, first, count):
        row, col, b1, _, _, _ = chunk(k)
        ref = at_out(row + core * half + b1 * quart + first * piece, count * piece, col)
        s = lax.rem(k, 8)
        return remote(ref, ref, gl_snd.at[s], gl_rcv.at[s], n_l)

    def gather_1(k):
        row, col, b1, _, to1, _ = chunk(k)
        ref = at_out(row + core * half + b1 * quart, quart, col)
        s = lax.rem(k, 8)
        return remote(ref, ref, a1_snd.at[s], a1_rcv.at[s], to1)

    def gather_d(k):
        row, col, _, _, _, _ = chunk(k)
        ref = at_out(row + core * half, half, col)
        s = lax.rem(k, 8)
        return remote(ref, ref, ad_snd.at[s], ad_rcv.at[s], n_d)

    blk = piece

    def e12(k):
        gather_d(k).wait_recv()
        gather_1(k).wait_send()
        gather_d(k).wait_send()
        for zz, right, left in ((0, (0, 1), None), (1, (0, 2), (1, 3)), (2, (0, 3), (2, 2)), (3, None, (3, 1))):

            @pl.when(z == zz)
            def _(right=right, left=left):
                if right:
                    gather_r(k, *right).wait_send()
                if left:
                    gather_l(k, *left).wait_send()

    def e11(k):
        gather_1(k).wait_recv()
        gather_d(k).start()

    def e10(k):
        @pl.when(z == 3)
        def _():
            gather_r(k, 0, 3).wait_recv()

        @pl.when(z == 0)
        def _():
            gather_l(k, 1, 3).wait_recv()

        gather_1(k).start()

    def e9(k):
        @pl.when(z == 2)
        def _():
            gather_r(k, 0, 2).wait_recv()
            gather_r(k, 0, 3).start()

        @pl.when(z == 1)
        def _():
            gather_l(k, 2, 2).wait_recv()
            gather_l(k, 1, 3).start()

    def e8(k):
        gather_3(k).wait_send()

        @pl.when(z == 1)
        def _():
            gather_r(k, 0, 1).wait_recv()
            gather_r(k, 0, 2).start()

        @pl.when(z == 2)
        def _():
            gather_l(k, 3, 1).wait_recv()
            gather_l(k, 2, 2).start()

    def e7(k):
        keep_final(k).wait()
        gather_3(k).wait_recv()

        @pl.when(z == 0)
        def _():
            gather_r(k, 0, 1).start()

        @pl.when(z == 3)
        def _():
            gather_l(k, 3, 1).start()

    def e6(k):
        s = lax.rem(k, 8)
        _, _, _, b3, _, _ = chunk(k)
        send_3(k).wait()
        mine = s2.at[s, pl.ds(pl.multiple_of(z * piece + b3 * last, last), last)]
        add_rows(mine, mine, r_3.at[lax.rem(k, 4)], last, last)
        for zz, right, left in (
            (0, (1, 3), None), (1, (2, 2), (0, 1)), (2, (3, 1), (0, 2)), (3, None, (0, 3)),
        ):

            @pl.when(z == zz)
            def _(right=right, left=left):
                if right:
                    send_zr(k, right[0] * piece, right[1] * piece).wait_send()
                if left:
                    send_zl(k, left[0] * piece, left[1] * piece).wait_send()

        keep_final(k).start()
        gather_3(k).start()

    def add_piece(k, buf, first, count):
        s = lax.rem(k, 8)
        mine = s2.at[s, pl.ds(first * piece, count * piece)]
        add_rows(mine, mine, buf.at[s, pl.ds(0, count * piece)], count * piece, blk)

    def e5(k):
        @pl.when(z == 3)
        def _():
            send_zr(k, 3 * piece, piece).wait_recv()
            add_piece(k, z_r, 3, 1)

        @pl.when(z == 0)
        def _():
            send_zl(k, 0, piece).wait_recv()
            add_piece(k, z_l, 0, 1)

        send_3(k).start()

    def e4(k):
        @pl.when(z == 2)
        def _():
            send_zr(k, 2 * piece, 2 * piece).wait_recv()
            add_piece(k, z_r, 2, 2)
            send_zr(k, 3 * piece, piece).start()

        @pl.when(z == 1)
        def _():
            send_zl(k, 0, 2 * piece).wait_recv()
            add_piece(k, z_l, 0, 2)
            send_zl(k, 0, piece).start()

    def e3(k):
        @pl.when(z == 1)
        def _():
            send_zr(k, piece, 3 * piece).wait_recv()
            add_piece(k, z_r, 1, 3)
            send_zr(k, 2 * piece, 2 * piece).start()

        @pl.when(z == 2)
        def _():
            send_zl(k, 0, 3 * piece).wait_recv()
            add_piece(k, z_l, 0, 3)
            send_zl(k, 0, 2 * piece).start()

    def e2(k):
        _, _, b1, _, _, _ = chunk(k)
        send_1(k).wait()
        kept = s1.at[lax.rem(k, 4), pl.ds(pl.multiple_of(b1 * quart, quart), quart)]
        add_rows(s2.at[lax.rem(k, 8)], kept, r_1.at[lax.rem(k, 8)], quart, blk)

        @pl.when(z == 0)
        def _():
            send_zr(k, piece, 3 * piece).start()

        @pl.when(z == 3)
        def _():
            send_zl(k, 0, 3 * piece).start()

    def e1(k):
        _, _, b1, _, _, _ = chunk(k)
        send_d(k).wait_recv()
        for b in (1 - b1, b1):
            r = pl.ds(pl.multiple_of(b * quart, quart), quart)
            own = pl.ds(pl.multiple_of(core * half + b * quart, quart), quart)
            add_rows(
                s1.at[lax.rem(k, 4), r], term.at[lax.rem(k, 2), own], r_d.at[lax.rem(k, 4), r], quart, blk
            )
        send_d(k).wait_send()
        send_1(k).start()

    def activation(q):
        wait(*gu_loads(q))

        @pl.when(q > 0)
        def _():
            h_store(q - 1).wait()

        step = min(16, qr)

        def body(i, _):
            r = pl.ds(pl.multiple_of(i * step, step), step)
            to = pl.ds(pl.multiple_of(q * qr + i * step, step), step)
            g, u, dh = g_buf[r].astype(F32), u_buf[r].astype(F32), acc[r]
            sig = jax.nn.sigmoid(g)
            silu = g * sig
            h_buf[r] = (silu * u).astype(BF)
            d[to, pl.ds(ff, ff)] = (dh * silu).astype(BF)
            d[to, pl.ds(0, ff)] = (dh * u * (sig + silu * (1.0 - sig))).astype(BF)

        lax.fori_loop(0, qr // step, body, None)
        h_store(q).start()

        @pl.when(q + 1 < QUARTERS)
        def _():
            go(*gu_loads(q + 1))

    def dh_tile(m):
        q, j, slot = lax.div(m, KBLOCKS), lax.rem(m, KBLOCKS), lax.rem(m, 2)
        wait(*dh_loads(m))
        acc[...] = jnp.where(j == 0, 0.0, acc[...]) + dot(dy_buf[slot], wd_buf[slot], NT)

        @pl.when(m + 2 < DH)
        def _():
            go(*dh_loads(m + 2))

        @pl.when(j == KBLOCKS - 1)
        def _():
            activation(q)

    def dx_tile(k):
        slot = lax.rem(k, 2)
        r = pl.ds(pl.multiple_of(lax.div(k, COLS) * qr, qr), qr)
        wait(*w_loads(k))
        term[slot] = dot(d[r], w_buf[slot], NT).astype(BF)

        @pl.when(k + 2 < CHUNKS)
        def _():
            go(*w_loads(k + 2))

    def dw_tile(u, j):
        slot = lax.rem(u, 2)

        @pl.when(j == 0)
        def _():
            x_load(u).wait()

        @pl.when(u > 0)
        def _():
            o_store(u - 1, j).wait()

        o_buf[j] = dot(x_buf[slot], d[:, pl.ds(pl.multiple_of(j * ff, ff), ff)], TN).astype(BF)
        o_store(u, j).start()

        @pl.when((j == 1) & (u + 2 < UNITS))
        def _():
            x_load(u + 2).start()

    def tick(t, _):
        g, s = lax.div(t, 4) - 1, lax.rem(t, 4)
        filler = 2 * g + s - 2

        @pl.when((t < FIRST) | ((s >= 2) & (filler < DH - KBLOCKS)))
        def _():
            dh_tile(jnp.where(t < FIRST, t, KBLOCKS + filler))

        @pl.when(t == FIRST)
        def _():
            go(x_load(0), x_load(1))

        @pl.when((t >= FIRST) & (s < 2) & (g < CHUNKS // 2))
        def _():
            dx_tile(2 * g + s)

        @pl.when((s >= 2) & (g >= DW_GROUP) & (g < DW_GROUP + UNITS))
        def _():
            dw_tile(g - DW_GROUP, s - 2)

        for off, event in (
            (E12, e12), (E11, e11), (E10, e10), (E9, e9), (E8, e8), (E7, e7), (E6, e6),
            (E5, e5), (E4, e4), (E3, e3), (E2, e2), (E1, e1), (0, lambda k: send_d(k).start()),
        ):
            at = t - FIRST - off
            k = 2 * lax.div(at, 4) + lax.rem(at, 4)

            @pl.when((at >= 0) & (lax.rem(at, 4) < 2) & (k < CHUNKS))
            def _(event=event, k=k):
                event(k)

    lax.fori_loop(0, TICKS, tick, None)
    h_store(QUARTERS - 1).wait()
    wait(o_store(UNITS - 1, 0), o_store(UNITS - 1, 1))


def main_call(x, dy, gate, up, w_gate, w_up, w_down):
    rows, cols = dy.shape
    ff = gate.shape[1]
    qr, nc, kb, xt = rows // QUARTERS, cols // COLS, cols // KBLOCKS, cols // UNITS
    half, quart, piece, last = qr // 2, qr // 4, qr // 16, qr // 32
    dma = pltpu.SemaphoreType.DMA
    vmem = pltpu.VMEM
    anywhere = pl.BlockSpec(memory_space=pl.ANY)
    flops = 2 * rows * cols * ff * 5
    return pl.pallas_call(
        main_kernel,
        out_shape=(
            jax.ShapeDtypeStruct((rows, cols), BF),
            jax.ShapeDtypeStruct((rows, ff), BF),
            jax.ShapeDtypeStruct((2, cols, ff), BF),
        ),
        in_specs=[anywhere] * 7,
        out_specs=(anywhere,) * 3,
        scratch_shapes=[
            vmem((rows, 2 * ff), BF),
            vmem((2, nc, 2 * ff), BF),
            vmem((2, ff, kb), BF),
            vmem((2, qr, kb), BF),
            vmem((2, rows, xt), BF),
            vmem((qr, ff), BF),
            vmem((qr, ff), BF),
            vmem((qr, ff), F32),
            vmem((qr, ff), BF),
            vmem((2, xt, ff), BF),
            vmem((2, qr, nc), BF),
            vmem((4, half, nc), BF),
            vmem((4, half, nc), BF),
            vmem((8, quart, nc), BF),
            vmem((8, quart, nc), BF),
            vmem((8, 3 * piece, nc), BF),
            vmem((8, 3 * piece, nc), BF),
            vmem((4, last, nc), BF),
            dma((2, 2)), dma((2, 2)), dma((2,)), dma((2,)), dma, dma((2,)), dma((4,)),
            dma((2,)), dma((4,)), dma((4,)), dma((8,)),
            dma((8,)), dma((8,)), dma((8,)), dma((8,)), dma((4,)), dma((4,)),
            dma((8,)), dma((8,)), dma((8,)), dma((8,)), dma((8,)), dma((8,)),
            dma((8,)), dma((8,)), dma((8,)), dma((8,)),
        ],
        compiler_params=pltpu.CompilerParams(
            collective_id=0, has_side_effects=True, vmem_limit_bytes=64_000_000
        ),
        cost_estimate=pl.CostEstimate(flops=flops, bytes_accessed=400 << 20, transcendentals=rows * ff),
        name="dx_reduce",
    )(x, dy, gate, up, w_gate, w_up, w_down)


def tail_kernel(hid, dy, dx_in, dw_in, dx, dw_gate, dw_up, dw_down):
    dw_down[...] = dot(hid[...], dy[...], TN).astype(BF)
    dx[...] = dx_in[...]
    dw_gate[...] = dw_in[0]
    dw_up[...] = dw_in[1]


def tail_call(hid, dy, dx, dw):
    rows, cols = dy.shape
    ff = hid.shape[1]
    n = UNITS
    spec = pl.BlockSpec
    return pl.pallas_call(
        tail_kernel,
        grid=(n,),
        out_shape=(
            jax.ShapeDtypeStruct((rows, cols), BF),
            jax.ShapeDtypeStruct((cols, ff), BF),
            jax.ShapeDtypeStruct((cols, ff), BF),
            jax.ShapeDtypeStruct((ff, cols), BF),
        ),
        in_specs=[
            spec((rows, ff), lambda i: (0, 0)),
            spec((rows, cols // n), lambda i: (0, i)),
            spec((rows // n, cols), lambda i: (i, 0)),
            spec((2, cols // n, ff), lambda i: (0, i, 0)),
        ],
        out_specs=(
            spec((rows // n, cols), lambda i: (i, 0)),
            spec((cols // n, ff), lambda i: (i, 0)),
            spec((cols // n, ff), lambda i: (i, 0)),
            spec((ff, cols // n), lambda i: (0, i)),
        ),
        compiler_params=pltpu.CompilerParams(vmem_limit_bytes=60_000_000),
        cost_estimate=pl.CostEstimate(
            flops=2 * rows * cols * ff, bytes_accessed=180 << 20, transcendentals=0
        ),
        name="dw_down_and_copies",
    )(hid, dy, dx, dw)


def solution(mesh):
    def step(x, dy, gate, up, w_gate, w_up, w_down):
        dx, hid, dw = main_call(x, dy, gate, up, w_gate, w_up, w_down)
        return tail_call(hid, dy, dx, dw)

    tokens, columns, rows = P("dp", None), P(None, "tp"), P("tp", None)
    return jax.shard_map(
        step,
        mesh=mesh,
        in_specs=(tokens, tokens, P("dp", "tp"), P("dp", "tp"), columns, columns, rows),
        out_specs=(tokens, P("dp", "tp"), P("dp", "tp"), P(("dp", "tp"), None)),
        check_vma=False,
    )
```

```python
import jax
import jax.numpy as jnp
from jax import lax
from jax.experimental import pallas as pl
from jax.experimental.pallas import tpu as pltpu
from jax.sharding import PartitionSpec as P

BF, F32 = jnp.bfloat16, jnp.float32
MESH = pl.DeviceIdType.MESH
NT = (((1,), (1,)), ((), ()))
TN = (((0,), (0,)), ((), ()))

QUARTERS = 4
COLS = 8
CHUNKS = QUARTERS * COLS
KBLOCKS = 4
UNITS = 16
DH = QUARTERS * KBLOCKS
E1, E2, E3, E4, E5, E6, E7, E8, E9, E10, E11, E12 = 1, 4, 7, 9, 11, 12, 14, 16, 18, 23, 33, 38
FIRST = KBLOCKS
FILLERS = DH - KBLOCKS + 2 * UNITS
TICKS = FIRST + max(2 * FILLERS, 2 * CHUNKS + E12)


def dot(a, b, dims):
    return lax.dot_general(a, b, dims, preferred_element_type=F32)


def add_rows(dst, a, b, rows, block):
    def body(i, _):
        r = pl.ds(pl.multiple_of(i * block, block), block)
        dst[r] = (a[r].astype(F32) + b[r].astype(F32)).astype(BF)

    lax.fori_loop(0, rows // block, body, None)


def main_kernel(
    x, dy, gate, up, w_gate, w_up, w_down, dx, hid, dw,
    d, w_buf, wd_buf, dy_buf, x_buf, g_buf, u_buf, acc, h_buf, o_buf,
    term, r_d, s1, r_1, s2, z_r, z_l, r_3,
    w_sem, dh_sem, x_sem, gu_sem, h_sem, o_sem, loc_sem,
    d_snd, d_rcv, s1_snd, s1_rcv, zr_snd, zr_rcv, zl_snd, zl_rcv, s3_snd, s3_rcv,
    a3_snd, a3_rcv, gr_snd, gr_rcv, gl_snd, gl_rcv, a1_snd, a1_rcv, ad_snd, ad_rcv,
):
    rows, cols = dy.shape
    ff = gate.shape[1]
    qr, nc, kb, xt = rows // QUARTERS, cols // COLS, cols // KBLOCKS, cols // UNITS
    half, quart, piece, last = qr // 2, qr // 4, qr // 16, qr // 32

    me = lax.axis_index("tp")
    core, z = lax.rem(me, 2), lax.rem(lax.div(me, 2), 4)
    y, xx = lax.rem(lax.div(me, 8), 2), lax.div(me, 16)
    n_d = me + 1 - 2 * core
    n_x, n_y = me + 16 * (1 - 2 * xx), me + 8 * (1 - 2 * y)
    n_r, n_l = me + 2, me - 2

    def copy(src, dst, sem):
        return pltpu.make_async_copy(src, dst, sem)

    def remote(src, dst, snd, rcv, to):
        return pltpu.make_async_remote_copy(
            src_ref=src, dst_ref=dst, send_sem=snd, recv_sem=rcv,
            device_id={"tp": to}, device_id_type=MESH,
        )

    def dh_loads(m):
        q, j, slot = lax.div(m, KBLOCKS), lax.rem(m, KBLOCKS), lax.rem(m, 2)
        k = pl.ds(pl.multiple_of(j * kb, kb), kb)
        r = pl.ds(pl.multiple_of(q * qr, qr), qr)
        return (
            copy(dy.at[r, k], dy_buf.at[slot], dh_sem.at[0, slot]),
            copy(w_down.at[:, k], wd_buf.at[slot], dh_sem.at[1, slot]),
        )

    def gu_loads(q):
        r = pl.ds(pl.multiple_of(q * qr, qr), qr)
        return copy(gate.at[r], g_buf, gu_sem.at[0]), copy(up.at[r], u_buf, gu_sem.at[1])

    def w_loads(k):
        slot = lax.rem(k, 2)
        r = pl.ds(pl.multiple_of(lax.rem(k, COLS) * nc, nc), nc)
        return (
            copy(w_gate.at[r], w_buf.at[slot, :, pl.ds(0, ff)], w_sem.at[0, slot]),
            copy(w_up.at[r], w_buf.at[slot, :, pl.ds(ff, ff)], w_sem.at[1, slot]),
        )

    def x_load(u):
        slot = lax.rem(u, 2)
        return copy(x.at[:, pl.ds(pl.multiple_of(u * xt, xt), xt)], x_buf.at[slot], x_sem.at[slot])

    def o_store(u, j):
        return copy(o_buf.at[j], dw.at[j, pl.ds(pl.multiple_of(u * xt, xt), xt)], o_sem.at[j])

    def h_store(q):
        return copy(h_buf, hid.at[pl.ds(pl.multiple_of(q * qr, qr), qr)], h_sem)

    def go(*copies):
        for c in copies:
            c.start()

    def wait(*copies):
        for c in copies:
            c.wait()

    go(*dh_loads(0))
    go(*dh_loads(1))
    go(*gu_loads(0))
    go(*w_loads(0))
    go(*w_loads(1))

    barrier = pltpu.get_barrier_semaphore()
    for to in (n_d, n_x, n_y):
        pl.semaphore_signal(barrier, inc=1, device_id={"tp": to}, device_id_type=MESH)

    @pl.when(z > 0)
    def _():
        pl.semaphore_signal(barrier, inc=1, device_id={"tp": n_l}, device_id_type=MESH)

    @pl.when(z < 3)
    def _():
        pl.semaphore_signal(barrier, inc=1, device_id={"tp": n_r}, device_id_type=MESH)

    pl.semaphore_wait(barrier, jnp.where((z > 0) & (z < 3), 5, 4))

    def chunk(k):
        q, n, odd = lax.div(k, COLS), lax.rem(k, COLS), lax.rem(k, 2)
        b1, b3 = jnp.where(odd == 0, xx, y), jnp.where(odd == 0, y, xx)
        to1, to3 = jnp.where(odd == 0, n_x, n_y), jnp.where(odd == 0, n_y, n_x)
        return q * qr, n * nc, b1, b3, to1, to3

    def at_out(row, count, col):
        return dx.at[pl.ds(pl.multiple_of(row, last), count), pl.ds(pl.multiple_of(col, nc), nc)]

    def send_d(k):
        s = lax.rem(k, 2)
        src = term.at[s, pl.ds(pl.multiple_of((1 - core) * half, half), half)]
        return remote(src, r_d.at[lax.rem(k, 4)], d_snd.at[s], d_rcv.at[lax.rem(k, 4)], n_d)

    def send_1(k):
        _, _, b1, _, to1, _ = chunk(k)
        src = s1.at[lax.rem(k, 4), pl.ds(pl.multiple_of((1 - b1) * quart, quart), quart)]
        return remote(src, r_1.at[lax.rem(k, 8)], s1_snd.at[lax.rem(k, 4)], s1_rcv.at[lax.rem(k, 8)], to1)

    def send_zr(k, row, count):
        s = lax.rem(k, 8)
        return remote(s2.at[s, pl.ds(row, count)], z_r.at[s, pl.ds(0, count)], zr_snd.at[s], zr_rcv.at[s], n_r)

    def send_zl(k, row, count):
        s = lax.rem(k, 8)
        return remote(s2.at[s, pl.ds(row, count)], z_l.at[s, pl.ds(0, count)], zl_snd.at[s], zl_rcv.at[s], n_l)

    def send_3(k):
        _, _, _, b3, _, to3 = chunk(k)
        src = s2.at[lax.rem(k, 8), pl.ds(pl.multiple_of(z * piece + (1 - b3) * last, last), last)]
        return remote(src, r_3.at[lax.rem(k, 4)], s3_snd.at[lax.rem(k, 4)], s3_rcv.at[lax.rem(k, 4)], to3)

    def final_rows(k):
        row, col, b1, b3, _, _ = chunk(k)
        return (
            s2.at[lax.rem(k, 8), pl.ds(pl.multiple_of(z * piece + b3 * last, last), last)],
            at_out(row + core * half + b1 * quart + z * piece + b3 * last, last, col),
        )

    def keep_final(k):
        src, dst = final_rows(k)
        return copy(src, dst, loc_sem.at[lax.rem(k, 4)])

    def gather_3(k):
        src, dst = final_rows(k)
        s = lax.rem(k, 8)
        return remote(src, dst, a3_snd.at[s], a3_rcv.at[s], chunk(k)[5])

    def gather_r(k, first, count):
        row, col, b1, _, _, _ = chunk(k)
        ref = at_out(row + core * half + b1 * quart + first * piece, count * piece, col)
        s = lax.rem(k, 8)
        return remote(ref, ref, gr_snd.at[s], gr_rcv.at[s], n_r)

    def gather_l(k, first, count):
        row, col, b1, _, _, _ = chunk(k)
        ref = at_out(row + core * half + b1 * quart + first * piece, count * piece, col)
        s = lax.rem(k, 8)
        return remote(ref, ref, gl_snd.at[s], gl_rcv.at[s], n_l)

    def gather_1(k):
        row, col, b1, _, to1, _ = chunk(k)
        ref = at_out(row + core * half + b1 * quart, quart, col)
        s = lax.rem(k, 16)
        return remote(ref, ref, a1_snd.at[s], a1_rcv.at[s], to1)

    def gather_d(k):
        row, col, _, _, _, _ = chunk(k)
        ref = at_out(row + core * half, half, col)
        s = lax.rem(k, 16)
        return remote(ref, ref, ad_snd.at[s], ad_rcv.at[s], n_d)

    blk = piece

    def e12(k):
        gather_d(k).wait_recv()
        gather_1(k).wait_send()
        gather_d(k).wait_send()
        for zz, right, left in ((0, (0, 1), None), (1, (0, 2), (1, 3)), (2, (0, 3), (2, 2)), (3, None, (3, 1))):

            @pl.when(z == zz)
            def _(right=right, left=left):
                if right:
                    gather_r(k, *right).wait_send()
                if left:
                    gather_l(k, *left).wait_send()

    def e11(k):
        gather_1(k).wait_recv()
        gather_d(k).start()

    def e10(k):
        @pl.when(z == 3)
        def _():
            gather_r(k, 0, 3).wait_recv()

        @pl.when(z == 0)
        def _():
            gather_l(k, 1, 3).wait_recv()

        gather_1(k).start()

    def e9(k):
        @pl.when(z == 2)
        def _():
            gather_r(k, 0, 2).wait_recv()
            gather_r(k, 0, 3).start()

        @pl.when(z == 1)
        def _():
            gather_l(k, 2, 2).wait_recv()
            gather_l(k, 1, 3).start()

    def e8(k):
        gather_3(k).wait_send()

        @pl.when(z == 1)
        def _():
            gather_r(k, 0, 1).wait_recv()
            gather_r(k, 0, 2).start()

        @pl.when(z == 2)
        def _():
            gather_l(k, 3, 1).wait_recv()
            gather_l(k, 2, 2).start()

    def e7(k):
        keep_final(k).wait()
        gather_3(k).wait_recv()

        @pl.when(z == 0)
        def _():
            gather_r(k, 0, 1).start()

        @pl.when(z == 3)
        def _():
            gather_l(k, 3, 1).start()

    def e6(k):
        s = lax.rem(k, 8)
        _, _, _, b3, _, _ = chunk(k)
        send_3(k).wait()
        mine = s2.at[s, pl.ds(pl.multiple_of(z * piece + b3 * last, last), last)]
        add_rows(mine, mine, r_3.at[lax.rem(k, 4)], last, last)
        for zz, right, left in (
            (0, (1, 3), None), (1, (2, 2), (0, 1)), (2, (3, 1), (0, 2)), (3, None, (0, 3)),
        ):

            @pl.when(z == zz)
            def _(right=right, left=left):
                if right:
                    send_zr(k, right[0] * piece, right[1] * piece).wait_send()
                if left:
                    send_zl(k, left[0] * piece, left[1] * piece).wait_send()

        keep_final(k).start()
        gather_3(k).start()

    def add_piece(k, buf, first, count):
        s = lax.rem(k, 8)
        mine = s2.at[s, pl.ds(first * piece, count * piece)]
        add_rows(mine, mine, buf.at[s, pl.ds(0, count * piece)], count * piece, blk)

    def e5(k):
        @pl.when(z == 3)
        def _():
            send_zr(k, 3 * piece, piece).wait_recv()
            add_piece(k, z_r, 3, 1)

        @pl.when(z == 0)
        def _():
            send_zl(k, 0, piece).wait_recv()
            add_piece(k, z_l, 0, 1)

        send_3(k).start()

    def e4(k):
        @pl.when(z == 2)
        def _():
            send_zr(k, 2 * piece, 2 * piece).wait_recv()
            add_piece(k, z_r, 2, 2)
            send_zr(k, 3 * piece, piece).start()

        @pl.when(z == 1)
        def _():
            send_zl(k, 0, 2 * piece).wait_recv()
            add_piece(k, z_l, 0, 2)
            send_zl(k, 0, piece).start()

    def e3(k):
        @pl.when(z == 1)
        def _():
            send_zr(k, piece, 3 * piece).wait_recv()
            add_piece(k, z_r, 1, 3)
            send_zr(k, 2 * piece, 2 * piece).start()

        @pl.when(z == 2)
        def _():
            send_zl(k, 0, 3 * piece).wait_recv()
            add_piece(k, z_l, 0, 3)
            send_zl(k, 0, 2 * piece).start()

    def e2(k):
        _, _, b1, _, _, _ = chunk(k)
        send_1(k).wait()
        kept = s1.at[lax.rem(k, 4), pl.ds(pl.multiple_of(b1 * quart, quart), quart)]
        add_rows(s2.at[lax.rem(k, 8)], kept, r_1.at[lax.rem(k, 8)], quart, blk)

        @pl.when(z == 0)
        def _():
            send_zr(k, piece, 3 * piece).start()

        @pl.when(z == 3)
        def _():
            send_zl(k, 0, 3 * piece).start()

    def e1(k):
        _, _, b1, _, _, _ = chunk(k)
        send_d(k).wait_recv()
        for b in (1 - b1, b1):
            r = pl.ds(pl.multiple_of(b * quart, quart), quart)
            own = pl.ds(pl.multiple_of(core * half + b * quart, quart), quart)
            add_rows(
                s1.at[lax.rem(k, 4), r], term.at[lax.rem(k, 2), own], r_d.at[lax.rem(k, 4), r], quart, blk
            )
        send_d(k).wait_send()
        send_1(k).start()

    def activation(q):
        wait(*gu_loads(q))

        @pl.when(q > 0)
        def _():
            h_store(q - 1).wait()

        step = min(16, qr)

        def body(i, _):
            r = pl.ds(pl.multiple_of(i * step, step), step)
            to = pl.ds(pl.multiple_of(q * qr + i * step, step), step)
            g, u, dh = g_buf[r].astype(F32), u_buf[r].astype(F32), acc[r]
            sig = jax.nn.sigmoid(g)
            silu = g * sig
            h_buf[r] = (silu * u).astype(BF)
            d[to, pl.ds(ff, ff)] = (dh * silu).astype(BF)
            d[to, pl.ds(0, ff)] = (dh * u * (sig + silu * (1.0 - sig))).astype(BF)

        lax.fori_loop(0, qr // step, body, None)
        h_store(q).start()

        @pl.when(q + 1 < QUARTERS)
        def _():
            go(*gu_loads(q + 1))

    def dh_tile(m):
        q, j, slot = lax.div(m, KBLOCKS), lax.rem(m, KBLOCKS), lax.rem(m, 2)
        wait(*dh_loads(m))
        acc[...] = jnp.where(j == 0, 0.0, acc[...]) + dot(dy_buf[slot], wd_buf[slot], NT)

        @pl.when(m + 2 < DH)
        def _():
            go(*dh_loads(m + 2))

        @pl.when(j == KBLOCKS - 1)
        def _():
            activation(q)

    def dx_tile(k):
        slot = lax.rem(k, 2)
        r = pl.ds(pl.multiple_of(lax.div(k, COLS) * qr, qr), qr)
        wait(*w_loads(k))
        term[slot] = dot(d[r], w_buf[slot], NT).astype(BF)

        @pl.when(k + 2 < CHUNKS)
        def _():
            go(*w_loads(k + 2))

    def dw_tile(u, j):
        slot = lax.rem(u, 2)

        @pl.when(j == 0)
        def _():
            x_load(u).wait()

        @pl.when(u > 0)
        def _():
            o_store(u - 1, j).wait()

        o_buf[j] = dot(x_buf[slot], d[:, pl.ds(pl.multiple_of(j * ff, ff), ff)], TN).astype(BF)
        o_store(u, j).start()

        @pl.when((j == 1) & (u + 2 < UNITS))
        def _():
            x_load(u + 2).start()

    def tick(t, _):
        i, s = lax.div(t - FIRST, 2), lax.rem(t, 2)

        @pl.when((t < FIRST) | ((s == 1) & (i < DH - KBLOCKS)))
        def _():
            dh_tile(jnp.where(t < FIRST, t, KBLOCKS + i))

        @pl.when(t == FIRST)
        def _():
            go(x_load(0), x_load(1))

        @pl.when((t >= FIRST) & (s == 0) & (i < CHUNKS))
        def _():
            dx_tile(i)

        w = i - (DH - KBLOCKS)

        @pl.when((s == 1) & (w >= 0) & (w < 2 * UNITS))
        def _():
            dw_tile(lax.div(w, 2), lax.rem(w, 2))

        for off, event in (
            (E12, e12), (E11, e11), (E10, e10), (E9, e9), (E8, e8), (E7, e7), (E6, e6),
            (E5, e5), (E4, e4), (E3, e3), (E2, e2), (E1, e1), (0, lambda k: send_d(k).start()),
        ):
            at = t - FIRST - off
            k = lax.div(at, 2)

            @pl.when((at >= 0) & (lax.rem(at, 2) == 0) & (k < CHUNKS))
            def _(event=event, k=k):
                event(k)

    lax.fori_loop(0, TICKS, tick, None)
    h_store(QUARTERS - 1).wait()
    wait(o_store(UNITS - 1, 0), o_store(UNITS - 1, 1))


def main_call(x, dy, gate, up, w_gate, w_up, w_down):
    rows, cols = dy.shape
    ff = gate.shape[1]
    qr, nc, kb, xt = rows // QUARTERS, cols // COLS, cols // KBLOCKS, cols // UNITS
    half, quart, piece, last = qr // 2, qr // 4, qr // 16, qr // 32
    dma = pltpu.SemaphoreType.DMA
    vmem = pltpu.VMEM
    anywhere = pl.BlockSpec(memory_space=pl.ANY)
    flops = 2 * rows * cols * ff * 5
    return pl.pallas_call(
        main_kernel,
        out_shape=(
            jax.ShapeDtypeStruct((rows, cols), BF),
            jax.ShapeDtypeStruct((rows, ff), BF),
            jax.ShapeDtypeStruct((2, cols, ff), BF),
        ),
        in_specs=[anywhere] * 7,
        out_specs=(anywhere,) * 3,
        scratch_shapes=[
            vmem((rows, 2 * ff), BF),
            vmem((2, nc, 2 * ff), BF),
            vmem((2, ff, kb), BF),
            vmem((2, qr, kb), BF),
            vmem((2, rows, xt), BF),
            vmem((qr, ff), BF),
            vmem((qr, ff), BF),
            vmem((qr, ff), F32),
            vmem((qr, ff), BF),
            vmem((2, xt, ff), BF),
            vmem((2, qr, nc), BF),
            vmem((4, half, nc), BF),
            vmem((4, half, nc), BF),
            vmem((8, quart, nc), BF),
            vmem((8, quart, nc), BF),
            vmem((8, 3 * piece, nc), BF),
            vmem((8, 3 * piece, nc), BF),
            vmem((4, last, nc), BF),
            dma((2, 2)), dma((2, 2)), dma((2,)), dma((2,)), dma, dma((2,)), dma((4,)),
            dma((2,)), dma((4,)), dma((4,)), dma((8,)),
            dma((8,)), dma((8,)), dma((8,)), dma((8,)), dma((4,)), dma((4,)),
            dma((8,)), dma((8,)), dma((8,)), dma((8,)), dma((8,)), dma((8,)),
            dma((16,)), dma((16,)), dma((16,)), dma((16,)),
        ],
        compiler_params=pltpu.CompilerParams(
            collective_id=0, has_side_effects=True, vmem_limit_bytes=64_000_000
        ),
        cost_estimate=pl.CostEstimate(flops=flops, bytes_accessed=400 << 20, transcendentals=rows * ff),
        name="dx_reduce",
    )(x, dy, gate, up, w_gate, w_up, w_down)


def tail_kernel(hid, dy, dx_in, dw_in, dx, dw_gate, dw_up, dw_down, dx_buf, dw_buf, in_sem, out_sem):
    i, n = pl.program_id(0), pl.num_programs(0)
    slots, dx_rows, _ = dx_buf.shape
    dw_rows = dw_buf.shape[2]

    def loads(j):
        s = lax.rem(j, slots)
        a = pl.ds(pl.multiple_of(j * dx_rows, dx_rows), dx_rows)
        b = pl.ds(pl.multiple_of(j * dw_rows, dw_rows), dw_rows)
        return (
            pltpu.make_async_copy(dx_in.at[a], dx_buf.at[s], in_sem.at[s, 0]),
            pltpu.make_async_copy(dw_in.at[0, b], dw_buf.at[s, 0], in_sem.at[s, 1]),
            pltpu.make_async_copy(dw_in.at[1, b], dw_buf.at[s, 1], in_sem.at[s, 2]),
        )

    def stores(j):
        s = lax.rem(j, slots)
        a = pl.ds(pl.multiple_of(j * dx_rows, dx_rows), dx_rows)
        b = pl.ds(pl.multiple_of(j * dw_rows, dw_rows), dw_rows)
        return (
            pltpu.make_async_copy(dx_buf.at[s], dx.at[a], out_sem.at[s, 0]),
            pltpu.make_async_copy(dw_buf.at[s, 0], dw_gate.at[b], out_sem.at[s, 1]),
            pltpu.make_async_copy(dw_buf.at[s, 1], dw_up.at[b], out_sem.at[s, 2]),
        )

    ahead = slots // 2

    @pl.when(i == 0)
    def _():
        for j in range(ahead):
            for c in loads(j):
                c.start()

    @pl.when(i >= ahead)
    def _():
        for c in stores(i - ahead):
            c.wait()

    @pl.when(i + ahead < n)
    def _():
        for c in loads(i + ahead):
            c.start()

    for c in loads(i):
        c.wait()
    for c in stores(i):
        c.start()
    dw_down[...] = dot(hid[...], dy[...], TN).astype(BF)

    @pl.when(i == n - 1)
    def _():
        for j in range(ahead):
            for c in stores(n - ahead + j):
                c.wait()


def tail_call(hid, dy, dx, dw):
    rows, cols = dy.shape
    ff = hid.shape[1]
    n, slots = UNITS, 4
    spec, anywhere = pl.BlockSpec, pl.BlockSpec(memory_space=pl.ANY)
    return pl.pallas_call(
        tail_kernel,
        grid=(n,),
        out_shape=(
            jax.ShapeDtypeStruct((rows, cols), BF),
            jax.ShapeDtypeStruct((cols, ff), BF),
            jax.ShapeDtypeStruct((cols, ff), BF),
            jax.ShapeDtypeStruct((ff, cols), BF),
        ),
        in_specs=[
            spec((rows, ff), lambda i: (0, 0)),
            spec((rows, cols // n), lambda i: (0, i)),
            anywhere,
            anywhere,
        ],
        out_specs=(anywhere, anywhere, anywhere, spec((ff, cols // n), lambda i: (0, i))),
        scratch_shapes=[
            pltpu.VMEM((slots, rows // n, cols), BF),
            pltpu.VMEM((slots, 2, cols // n, ff), BF),
            pltpu.SemaphoreType.DMA((slots, 3)),
            pltpu.SemaphoreType.DMA((slots, 3)),
        ],
        compiler_params=pltpu.CompilerParams(vmem_limit_bytes=60_000_000),
        cost_estimate=pl.CostEstimate(
            flops=2 * rows * cols * ff, bytes_accessed=180 << 20, transcendentals=0
        ),
        name="dw_down_and_copies",
    )(hid, dy, dx, dw)


def solution(mesh):
    def step(x, dy, gate, up, w_gate, w_up, w_down):
        dx, hid, dw = main_call(x, dy, gate, up, w_gate, w_up, w_down)
        return tail_call(hid, dy, dx, dw)

    tokens, columns, rows = P("dp", None), P(None, "tp"), P("tp", None)
    return jax.shard_map(
        step,
        mesh=mesh,
        in_specs=(tokens, tokens, P("dp", "tp"), P("dp", "tp"), columns, columns, rows),
        out_specs=(tokens, P("dp", "tp"), P("dp", "tp"), P(("dp", "tp"), None)),
        check_vma=False,
    )
```

```python
import jax
import jax.numpy as jnp
from jax import lax
from jax.experimental import pallas as pl
from jax.experimental.pallas import tpu as pltpu
from jax.sharding import PartitionSpec as P

BF, F32 = jnp.bfloat16, jnp.float32
MESH = pl.DeviceIdType.MESH
NT = (((1,), (1,)), ((), ()))
TN = (((0,), (0,)), ((), ()))

QUARTERS = 4
COLS = 8
TILES = QUARTERS * COLS
KBLOCKS = 4
UNITS = 16
DH = QUARTERS * KBLOCKS
FIRST = KBLOCKS
LEAD = 4
STEPS = dict(
    e1=(1, 15), e2=(3, 16), e3=(4, 16), e4=(6, 16), e5=(9, 16), e6=(14, 16),
    e8=(15, 16), e9=(19, 16), e10=(24, 17), e11=(35, 15), e12=(44, 16),
)
FILLERS = DH - KBLOCKS + 2 * UNITS
LAST_STEP = STEPS["e12"][0] + STEPS["e12"][1] * (TILES - 1) // 8
TICKS = FIRST + max(LEAD + 2 * FILLERS, LAST_STEP + 1)
N_TERM, N_RD, N_S1, N_R1, N_S2, N_Z, N_R3, N_SEM = 3, 4, 4, 6, 8, 8, 8, 16


def dot(a, b, dims):
    return lax.dot_general(a, b, dims, preferred_element_type=F32)


def add_rows(dst, a, b, rows, block):
    def body(i, _):
        r = pl.ds(pl.multiple_of(i * block, block), block)
        dst[r] = (a[r].astype(F32) + b[r].astype(F32)).astype(BF)

    lax.fori_loop(0, rows // block, body, None)


def main_kernel(
    x, dy, gate, up, w_gate, w_up, w_down, dx, hid, dw,
    d, w_buf, wd_buf, dy_buf, x_buf, g_buf, u_buf, acc, h_buf, o_buf,
    term, r_d, s1, r_1, s2, z_r, z_l, r_3,
    w_sem, dh_sem, x_sem, gu_sem, h_sem, o_sem, loc_sem,
    d_snd, d_rcv, s1_snd, s1_rcv, zr_snd, zr_rcv, zl_snd, zl_rcv, s3_snd, s3_rcv,
    gr_snd, gr_rcv, gl_snd, gl_rcv, a1_snd, a1_rcv, ad_snd, ad_rcv,
):
    rows, cols = dy.shape
    ff = gate.shape[1]
    qr, nc, kb, xt = rows // QUARTERS, cols // COLS, cols // KBLOCKS, cols // UNITS
    half, quart, piece = qr // 2, qr // 4, qr // 16

    me = lax.axis_index("tp")
    core, z = lax.rem(me, 2), lax.rem(lax.div(me, 2), 4)
    y, xx = lax.rem(lax.div(me, 8), 2), lax.div(me, 16)
    n_d = me + 1 - 2 * core
    n_x, n_y = me + 16 * (1 - 2 * xx), me + 8 * (1 - 2 * y)
    n_r, n_l = me + 2, me - 2

    def copy(src, dst, sem):
        return pltpu.make_async_copy(src, dst, sem)

    def remote(src, dst, snd, rcv, to):
        return pltpu.make_async_remote_copy(
            src_ref=src, dst_ref=dst, send_sem=snd, recv_sem=rcv,
            device_id={"tp": to}, device_id_type=MESH,
        )

    def dh_loads(m):
        q, j, slot = lax.div(m, KBLOCKS), lax.rem(m, KBLOCKS), lax.rem(m, 2)
        k = pl.ds(pl.multiple_of(j * kb, kb), kb)
        r = pl.ds(pl.multiple_of(q * qr, qr), qr)
        return (
            copy(dy.at[r, k], dy_buf.at[slot], dh_sem.at[0, slot]),
            copy(w_down.at[:, k], wd_buf.at[slot], dh_sem.at[1, slot]),
        )

    def gu_loads(q):
        r = pl.ds(pl.multiple_of(q * qr, qr), qr)
        return copy(gate.at[r], g_buf, gu_sem.at[0]), copy(up.at[r], u_buf, gu_sem.at[1])

    def w_loads(k):
        slot = lax.rem(k, 2)
        r = pl.ds(pl.multiple_of(lax.rem(k, COLS) * nc, nc), nc)
        return (
            copy(w_gate.at[r], w_buf.at[slot, :, pl.ds(0, ff)], w_sem.at[0, slot]),
            copy(w_up.at[r], w_buf.at[slot, :, pl.ds(ff, ff)], w_sem.at[1, slot]),
        )

    def x_load(u):
        slot = lax.rem(u, 2)
        return copy(x.at[:, pl.ds(pl.multiple_of(u * xt, xt), xt)], x_buf.at[slot], x_sem.at[slot])

    def o_store(u, j):
        return copy(o_buf.at[j], dw.at[j, pl.ds(pl.multiple_of(u * xt, xt), xt)], o_sem.at[j])

    def h_store(q):
        return copy(h_buf, hid.at[pl.ds(pl.multiple_of(q * qr, qr), qr)], h_sem)

    def go(*copies):
        for c in copies:
            c.start()

    def wait(*copies):
        for c in copies:
            c.wait()

    go(*dh_loads(0))
    go(*dh_loads(1))
    go(*gu_loads(0))
    go(*w_loads(0))
    go(*w_loads(1))

    barrier = pltpu.get_barrier_semaphore()
    for to in (n_d, n_x, n_y):
        pl.semaphore_signal(barrier, inc=1, device_id={"tp": to}, device_id_type=MESH)

    @pl.when(z > 0)
    def _():
        pl.semaphore_signal(barrier, inc=1, device_id={"tp": n_l}, device_id_type=MESH)

    @pl.when(z < 3)
    def _():
        pl.semaphore_signal(barrier, inc=1, device_id={"tp": n_r}, device_id_type=MESH)

    pl.semaphore_wait(barrier, jnp.where((z > 0) & (z < 3), 5, 4))

    first_bit, third_bit = (xx, y), (y, xx)
    first_to, third_to = (n_x, n_y), (n_y, n_x)
    hc = nc // 2

    def at_out(i, c, row, count, width=hc):
        r = lax.div(i, COLS) * qr + core * half + row
        k = lax.rem(i, COLS) * nc + c * hc
        return dx.at[pl.ds(pl.multiple_of(r, piece), count), pl.ds(pl.multiple_of(k, hc), width)]

    def slot_of(i, count):
        return lax.rem(i, count)

    def send_d(i):
        s, t = slot_of(i, N_TERM), slot_of(i, N_RD)
        src = term.at[s, pl.ds(pl.multiple_of((1 - core) * half, half), half)]
        return remote(src, r_d.at[t], d_snd.at[s], d_rcv.at[t], n_d)

    def send_1(i, c):
        s, t = slot_of(i, N_S1), slot_of(i, N_R1)
        src = s1.at[s, c, pl.ds(pl.multiple_of((1 - first_bit[c]) * quart, quart), quart)]
        return remote(src, r_1.at[t, c], s1_snd.at[s, c], s1_rcv.at[t, c], first_to[c])

    def send_z(i, c, right, row, count):
        s, t = slot_of(i, N_S2), slot_of(i, N_Z)
        src = s2.at[s, c, pl.ds(row * piece, count * piece)]
        buf, snd, rcv, to = (z_r, zr_snd, zr_rcv, n_r) if right else (z_l, zl_snd, zl_rcv, n_l)
        return remote(src, buf.at[t, c, pl.ds(0, count * piece)], snd.at[t, c], rcv.at[t, c], to)

    def own_piece(i, c):
        return s2.at[slot_of(i, N_S2), c, pl.ds(pl.multiple_of(z * piece, piece), piece)]

    def send_3(i, c):
        t = slot_of(i, N_R3)
        return remote(own_piece(i, c), r_3.at[t, c], s3_snd.at[t, c], s3_rcv.at[t, c], third_to[c])

    def keep_final(i, c):
        out = at_out(i, c, first_bit[c] * quart + z * piece, piece)
        return copy(own_piece(i, c), out, loc_sem.at[slot_of(i, N_SEM), c])

    def gather_z(i, c, right, first, count, fresh=False):
        ref = at_out(i, c, first_bit[c] * quart + first * piece, count * piece)
        snd, rcv, to = (gr_snd, gr_rcv, n_r) if right else (gl_snd, gl_rcv, n_l)
        s = slot_of(i, N_SEM)
        return remote(own_piece(i, c) if fresh else ref, ref, snd.at[s, c], rcv.at[s, c], to)

    def gather_1(i, c):
        ref, s = at_out(i, c, first_bit[c] * quart, quart), slot_of(i, N_SEM)
        return remote(ref, ref, a1_snd.at[s, c], a1_rcv.at[s, c], first_to[c])

    def gather_d(i):
        ref, s = at_out(i, 0, 0, half, nc), slot_of(i, N_SEM)
        return remote(ref, ref, ad_snd.at[s], ad_rcv.at[s], n_d)

    def on_line(*cases):
        for zz, body in cases:

            @pl.when(z == zz)
            def _(body=body):
                body()

    def both(body):
        for c in (0, 1):
            body(c)

    def add_piece(i, c, right, first, count):
        buf = z_r if right else z_l
        mine = s2.at[slot_of(i, N_S2), c, pl.ds(first * piece, count * piece)]
        add_rows(mine, mine, buf.at[slot_of(i, N_Z), c, pl.ds(0, count * piece)], count * piece, piece)

    def e12(i):
        gather_d(i).wait()
        both(lambda c: gather_1(i, c).wait_send())

        def middle(rights, lefts):
            def body():
                for c in (0, 1):
                    gather_z(i, c, True, *rights).wait_send()
                    gather_z(i, c, False, *lefts).wait_send()

            return body

        on_line((1, middle((0, 2), (1, 3))), (2, middle((0, 3), (2, 2))))

    def e11(i):
        both(lambda c: gather_1(i, c).wait_recv())
        gather_d(i).start()

    def e10(i):
        on_line(
            (3, lambda: both(lambda c: gather_z(i, c, True, 0, 3).wait_recv())),
            (0, lambda: both(lambda c: gather_z(i, c, False, 1, 3).wait_recv())),
        )
        both(lambda c: gather_1(i, c).start())

    def pass_on(i, right, got, gives):
        def body():
            for c in (0, 1):
                gather_z(i, c, right, *got).wait_recv()
                gather_z(i, c, right, *gives).start()

        return body

    def e9(i):
        on_line((2, pass_on(i, True, (0, 2), (0, 3))), (1, pass_on(i, False, (2, 2), (1, 3))))

    def e8(i):
        both(lambda c: keep_final(i, c).wait())
        on_line(
            (0, lambda: both(lambda c: gather_z(i, c, True, 0, 1, True).wait_send())),
            (1, pass_on(i, True, (0, 1), (0, 2))),
            (2, pass_on(i, False, (3, 1), (2, 2))),
            (3, lambda: both(lambda c: gather_z(i, c, False, 3, 1, True).wait_send())),
        )

    def e6(i):
        for c in (0, 1):
            send_3(i, c).wait()
            add_rows(own_piece(i, c), own_piece(i, c), r_3.at[slot_of(i, N_R3), c], piece, piece)

        def sent(rights, lefts):
            def body():
                for c in (0, 1):
                    if rights:
                        send_z(i, c, True, *rights).wait_send()
                    if lefts:
                        send_z(i, c, False, *lefts).wait_send()

            return body

        on_line(
            (0, sent((1, 3), None)),
            (1, sent((2, 2), (0, 1))),
            (2, sent((3, 1), (0, 2))),
            (3, sent(None, (0, 3))),
        )
        both(lambda c: keep_final(i, c).start())
        on_line(
            (0, lambda: both(lambda c: gather_z(i, c, True, 0, 1, True).start())),
            (3, lambda: both(lambda c: gather_z(i, c, False, 3, 1, True).start())),
        )

    def take(i, right, first, count, gives=None):
        def body():
            for c in (0, 1):
                send_z(i, c, right, first, count).wait_recv()
                add_piece(i, c, right, first, count)
                if gives:
                    send_z(i, c, right, *gives).start()

        return body

    def e5(i):
        on_line((3, take(i, True, 3, 1)), (0, take(i, False, 0, 1)))
        both(lambda c: send_3(i, c).start())

    def e4(i):
        on_line((2, take(i, True, 2, 2, (3, 1))), (1, take(i, False, 0, 2, (0, 1))))

    def e3(i):
        on_line((1, take(i, True, 1, 3, (2, 2))), (2, take(i, False, 0, 3, (0, 2))))

    def e2(i):
        for c in (0, 1):
            send_1(i, c).wait()
            kept = s1.at[slot_of(i, N_S1), c, pl.ds(pl.multiple_of(first_bit[c] * quart, quart), quart)]
            add_rows(s2.at[slot_of(i, N_S2), c], kept, r_1.at[slot_of(i, N_R1), c], quart, piece)
            on_line(
                (0, lambda c=c: send_z(i, c, True, 1, 3).start()),
                (3, lambda c=c: send_z(i, c, False, 0, 3).start()),
            )

    def e1(i):
        send_d(i).wait_recv()
        got = r_d.at[slot_of(i, N_RD)]
        for part in (0, 1):
            for c in (0, 1):
                b = first_bit[c] if part else 1 - first_bit[c]
                r = pl.ds(pl.multiple_of(b * quart, quart), quart)
                own = pl.ds(pl.multiple_of(core * half + b * quart, quart), quart)
                k = pl.ds(c * hc, hc)
                add_rows(
                    s1.at[slot_of(i, N_S1), c, r], term.at[slot_of(i, N_TERM), own, k], got.at[r, k], quart, piece
                )
        send_d(i).wait_send()
        both(lambda c: send_1(i, c).start())

    def e0(i):
        send_d(i).start()

    def activation(q):
        wait(*gu_loads(q))

        @pl.when(q > 0)
        def _():
            h_store(q - 1).wait()

        step = min(16, qr)

        def body(i, _):
            r = pl.ds(pl.multiple_of(i * step, step), step)
            to = pl.ds(pl.multiple_of(q * qr + i * step, step), step)
            g, u, dh = g_buf[r].astype(F32), u_buf[r].astype(F32), acc[r]
            sig = jax.nn.sigmoid(g)
            silu = g * sig
            h_buf[r] = (silu * u).astype(BF)
            d[to, pl.ds(ff, ff)] = (dh * silu).astype(BF)
            d[to, pl.ds(0, ff)] = (dh * u * (sig + silu * (1.0 - sig))).astype(BF)

        lax.fori_loop(0, qr // step, body, None)
        h_store(q).start()

        @pl.when(q + 1 < QUARTERS)
        def _():
            go(*gu_loads(q + 1))

    def dh_tile(m):
        q, j, slot = lax.div(m, KBLOCKS), lax.rem(m, KBLOCKS), lax.rem(m, 2)
        wait(*dh_loads(m))
        acc[...] = jnp.where(j == 0, 0.0, acc[...]) + dot(dy_buf[slot], wd_buf[slot], NT)

        @pl.when(m + 2 < DH)
        def _():
            go(*dh_loads(m + 2))

        @pl.when(j == KBLOCKS - 1)
        def _():
            activation(q)

    def dx_tile(k):
        slot = lax.rem(k, 2)
        r = pl.ds(pl.multiple_of(lax.div(k, COLS) * qr, qr), qr)
        wait(*w_loads(k))
        term[lax.rem(k, N_TERM)] = dot(d[r], w_buf[slot], NT).astype(BF)

        @pl.when(k + 2 < TILES)
        def _():
            go(*w_loads(k + 2))

    def dw_tile(u, j):
        slot = lax.rem(u, 2)

        @pl.when(j == 0)
        def _():
            x_load(u).wait()

        @pl.when(u > 0)
        def _():
            o_store(u - 1, j).wait()

        o_buf[j] = dot(x_buf[slot], d[:, pl.ds(pl.multiple_of(j * ff, ff), ff)], TN).astype(BF)
        o_store(u, j).start()

        @pl.when((j == 1) & (u + 2 < UNITS))
        def _():
            x_load(u + 2).start()

    steps = dict(e1=e1, e2=e2, e3=e3, e4=e4, e5=e5, e6=e6, e8=e8, e9=e9, e10=e10, e11=e11, e12=e12)

    def tick(t, _):
        n = t - FIRST - LEAD
        i, odd = lax.div(n, 2), lax.rem(n, 2)

        @pl.when((t < FIRST) | ((odd == 1) & (i < DH - KBLOCKS)))
        def _():
            dh_tile(jnp.where(t < FIRST, t, KBLOCKS + i))

        @pl.when(t == FIRST)
        def _():
            go(x_load(0), x_load(1))

        tile = jnp.where(n < 0, t - FIRST, LEAD + i)
        has_tile = (t >= FIRST) & ((n < 0) | (odd == 0)) & (tile < TILES)

        @pl.when(has_tile)
        def _():
            dx_tile(tile)

        w = i - (DH - KBLOCKS)

        @pl.when((odd == 1) & (w >= 0) & (w < 2 * UNITS))
        def _():
            dw_tile(lax.div(w, 2), lax.rem(w, 2))

        for name, event in reversed(steps.items()):
            base, pace = STEPS[name]
            at = t - FIRST - base
            j = lax.div(at * 8 + pace - 1, pace)

            @pl.when((at >= 0) & (j < TILES) & (lax.div(j * pace, 8) == at))
            def _(event=event, j=j):
                event(j)

        @pl.when(has_tile)
        def _():
            e0(tile)

    lax.fori_loop(0, TICKS, tick, None)
    h_store(QUARTERS - 1).wait()
    wait(o_store(UNITS - 1, 0), o_store(UNITS - 1, 1))


def main_call(x, dy, gate, up, w_gate, w_up, w_down):
    rows, cols = dy.shape
    ff = gate.shape[1]
    qr, nc, kb, xt = rows // QUARTERS, cols // COLS, cols // KBLOCKS, cols // UNITS
    half, quart, piece, hc = qr // 2, qr // 4, qr // 16, nc // 2
    dma = pltpu.SemaphoreType.DMA
    vmem = pltpu.VMEM
    anywhere = pl.BlockSpec(memory_space=pl.ANY)
    flops = 2 * rows * cols * ff * 5
    return pl.pallas_call(
        main_kernel,
        out_shape=(
            jax.ShapeDtypeStruct((rows, cols), BF),
            jax.ShapeDtypeStruct((rows, ff), BF),
            jax.ShapeDtypeStruct((2, cols, ff), BF),
        ),
        in_specs=[anywhere] * 7,
        out_specs=(anywhere,) * 3,
        scratch_shapes=[
            vmem((rows, 2 * ff), BF),
            vmem((2, nc, 2 * ff), BF),
            vmem((2, ff, kb), BF),
            vmem((2, qr, kb), BF),
            vmem((2, rows, xt), BF),
            vmem((qr, ff), BF),
            vmem((qr, ff), BF),
            vmem((qr, ff), F32),
            vmem((qr, ff), BF),
            vmem((2, xt, ff), BF),
            vmem((N_TERM, qr, nc), BF),
            vmem((N_RD, half, nc), BF),
            vmem((N_S1, 2, half, hc), BF),
            vmem((N_R1, 2, quart, hc), BF),
            vmem((N_S2, 2, quart, hc), BF),
            vmem((N_Z, 2, 3 * piece, hc), BF),
            vmem((N_Z, 2, 3 * piece, hc), BF),
            vmem((N_R3, 2, piece, hc), BF),
            dma((2, 2)), dma((2, 2)), dma((2,)), dma((2,)), dma, dma((2,)), dma((N_SEM, 2)),
            dma((N_TERM,)), dma((N_RD,)), dma((N_S1, 2)), dma((N_R1, 2)),
            dma((N_Z, 2)), dma((N_Z, 2)), dma((N_Z, 2)), dma((N_Z, 2)), dma((N_R3, 2)), dma((N_R3, 2)),
            dma((N_SEM, 2)), dma((N_SEM, 2)), dma((N_SEM, 2)), dma((N_SEM, 2)),
            dma((N_SEM, 2)), dma((N_SEM, 2)), dma((N_SEM,)), dma((N_SEM,)),
        ],
        compiler_params=pltpu.CompilerParams(
            collective_id=0, has_side_effects=True, vmem_limit_bytes=64_000_000
        ),
        cost_estimate=pl.CostEstimate(flops=flops, bytes_accessed=400 << 20, transcendentals=rows * ff),
        name="dx_reduce",
    )(x, dy, gate, up, w_gate, w_up, w_down)


def tail_kernel(hid, dy, dx_in, dw_in, dx, dw_gate, dw_up, dw_down, dx_buf, dw_buf, in_sem, out_sem):
    i, n = pl.program_id(0), pl.num_programs(0)
    slots, dx_rows, _ = dx_buf.shape
    dw_rows = dw_buf.shape[2]

    def loads(j):
        s = lax.rem(j, slots)
        a = pl.ds(pl.multiple_of(j * dx_rows, dx_rows), dx_rows)
        b = pl.ds(pl.multiple_of(j * dw_rows, dw_rows), dw_rows)
        return (
            pltpu.make_async_copy(dx_in.at[a], dx_buf.at[s], in_sem.at[s, 0]),
            pltpu.make_async_copy(dw_in.at[0, b], dw_buf.at[s, 0], in_sem.at[s, 1]),
            pltpu.make_async_copy(dw_in.at[1, b], dw_buf.at[s, 1], in_sem.at[s, 2]),
        )

    def stores(j):
        s = lax.rem(j, slots)
        a = pl.ds(pl.multiple_of(j * dx_rows, dx_rows), dx_rows)
        b = pl.ds(pl.multiple_of(j * dw_rows, dw_rows), dw_rows)
        return (
            pltpu.make_async_copy(dx_buf.at[s], dx.at[a], out_sem.at[s, 0]),
            pltpu.make_async_copy(dw_buf.at[s, 0], dw_gate.at[b], out_sem.at[s, 1]),
            pltpu.make_async_copy(dw_buf.at[s, 1], dw_up.at[b], out_sem.at[s, 2]),
        )

    ahead = slots // 2

    @pl.when(i == 0)
    def _():
        for j in range(ahead):
            for c in loads(j):
                c.start()

    @pl.when(i >= ahead)
    def _():
        for c in stores(i - ahead):
            c.wait()

    @pl.when(i + ahead < n)
    def _():
        for c in loads(i + ahead):
            c.start()

    for c in loads(i):
        c.wait()
    for c in stores(i):
        c.start()
    dw_down[...] = dot(hid[...], dy[...], TN).astype(BF)

    @pl.when(i == n - 1)
    def _():
        for j in range(ahead):
            for c in stores(n - ahead + j):
                c.wait()


def tail_call(hid, dy, dx, dw):
    rows, cols = dy.shape
    ff = hid.shape[1]
    n, slots = UNITS, 4
    spec, anywhere = pl.BlockSpec, pl.BlockSpec(memory_space=pl.ANY)
    return pl.pallas_call(
        tail_kernel,
        grid=(n,),
        out_shape=(
            jax.ShapeDtypeStruct((rows, cols), BF),
            jax.ShapeDtypeStruct((cols, ff), BF),
            jax.ShapeDtypeStruct((cols, ff), BF),
            jax.ShapeDtypeStruct((ff, cols), BF),
        ),
        in_specs=[
            spec((rows, ff), lambda i: (0, 0)),
            spec((rows, cols // n), lambda i: (0, i)),
            anywhere,
            anywhere,
        ],
        out_specs=(anywhere, anywhere, anywhere, spec((ff, cols // n), lambda i: (0, i))),
        scratch_shapes=[
            pltpu.VMEM((slots, rows // n, cols), BF),
            pltpu.VMEM((slots, 2, cols // n, ff), BF),
            pltpu.SemaphoreType.DMA((slots, 3)),
            pltpu.SemaphoreType.DMA((slots, 3)),
        ],
        compiler_params=pltpu.CompilerParams(vmem_limit_bytes=60_000_000),
        cost_estimate=pl.CostEstimate(
            flops=2 * rows * cols * ff, bytes_accessed=180 << 20, transcendentals=0
        ),
        name="dw_down_and_copies",
    )(hid, dy, dx, dw)


def solution(mesh):
    def step(x, dy, gate, up, w_gate, w_up, w_down):
        dx, hid, dw = main_call(x, dy, gate, up, w_gate, w_up, w_down)
        return tail_call(hid, dy, dx, dw)

    tokens, columns, rows = P("dp", None), P(None, "tp"), P("tp", None)
    return jax.shard_map(
        step,
        mesh=mesh,
        in_specs=(tokens, tokens, P("dp", "tp"), P("dp", "tp"), columns, columns, rows),
        out_specs=(tokens, P("dp", "tp"), P("dp", "tp"), P(("dp", "tp"), None)),
        check_vma=False,
    )
```

```python
import jax
import jax.numpy as jnp
from jax import lax
from jax.experimental import pallas as pl
from jax.experimental.pallas import tpu as pltpu
from jax.sharding import PartitionSpec as P

BF, F32 = jnp.bfloat16, jnp.float32
MESH = pl.DeviceIdType.MESH
NT = (((1,), (1,)), ((), ()))
TN = (((0,), (0,)), ((), ()))

QUARTERS = 4
COLS = 8
TILES = QUARTERS * COLS
KBLOCKS = 4
UNITS = 16
DH = QUARTERS * KBLOCKS
LEAD = 4
STEPS = dict(
    e1=3, e2=7, e3=9, e4=11, e5=13, e6=16, e8=18, e9=22, e10=30, e11=34, e12=38,
)
FILLERS = DH - KBLOCKS + 2 * UNITS
TRIPS = max(LEAD + FILLERS, TILES + STEPS["e12"] // 2 + 1)
N_TERM, N_RD, N_S1, N_R1, N_S2, N_Z, N_R3, N_SEM = 2, 4, 4, 8, 8, 8, 8, 16


def dot(a, b, dims):
    return lax.dot_general(a, b, dims, preferred_element_type=F32)


def add_rows(dst, a, b, rows, block):
    def body(i, _):
        r = pl.ds(pl.multiple_of(i * block, block), block)
        dst[r] = (a[r].astype(F32) + b[r].astype(F32)).astype(BF)

    lax.fori_loop(0, rows // block, body, None)


def main_kernel(
    x, dy, gate, up, w_gate, w_up, w_down, dx, hid, dw,
    d, w_buf, wd_buf, dy_buf, x_buf, g_buf, u_buf, acc, h_buf, o_buf,
    term, r_d, s1, r_1, s2, z_r, z_l, r_3,
    w_sem, dh_sem, x_sem, gu_sem, h_sem, o_sem, loc_sem,
    d_snd, d_rcv, s1_snd, s1_rcv, zr_snd, zr_rcv, zl_snd, zl_rcv, s3_snd, s3_rcv,
    gr_snd, gr_rcv, gl_snd, gl_rcv, a1_snd, a1_rcv, ad_snd, ad_rcv,
):
    rows, cols = dy.shape
    ff = gate.shape[1]
    qr, nc, kb, xt = rows // QUARTERS, cols // COLS, cols // KBLOCKS, cols // UNITS
    half, quart, piece = qr // 2, qr // 4, qr // 16

    me = lax.axis_index("tp")
    core, z = lax.rem(me, 2), lax.rem(lax.div(me, 2), 4)
    y, xx = lax.rem(lax.div(me, 8), 2), lax.div(me, 16)
    n_d = me + 1 - 2 * core
    n_x, n_y = me + 16 * (1 - 2 * xx), me + 8 * (1 - 2 * y)
    n_r, n_l = me + 2, me - 2

    def copy(src, dst, sem):
        return pltpu.make_async_copy(src, dst, sem)

    def remote(src, dst, snd, rcv, to):
        return pltpu.make_async_remote_copy(
            src_ref=src, dst_ref=dst, send_sem=snd, recv_sem=rcv,
            device_id={"tp": to}, device_id_type=MESH,
        )

    def dh_loads(m):
        q, j, slot = lax.div(m, KBLOCKS), lax.rem(m, KBLOCKS), lax.rem(m, 2)
        k = pl.ds(pl.multiple_of(j * kb, kb), kb)
        r = pl.ds(pl.multiple_of(q * qr, qr), qr)
        return (
            copy(dy.at[r, k], dy_buf.at[slot], dh_sem.at[0, slot]),
            copy(w_down.at[:, k], wd_buf.at[slot], dh_sem.at[1, slot]),
        )

    def gu_loads(q):
        r = pl.ds(pl.multiple_of(q * qr, qr), qr)
        return copy(gate.at[r], g_buf, gu_sem.at[0]), copy(up.at[r], u_buf, gu_sem.at[1])

    def w_loads(k):
        slot = lax.rem(k, 2)
        r = pl.ds(pl.multiple_of(lax.rem(k, COLS) * nc, nc), nc)
        return (
            copy(w_gate.at[r], w_buf.at[slot, :, pl.ds(0, ff)], w_sem.at[0, slot]),
            copy(w_up.at[r], w_buf.at[slot, :, pl.ds(ff, ff)], w_sem.at[1, slot]),
        )

    def x_load(u):
        slot = lax.rem(u, 2)
        return copy(x.at[:, pl.ds(pl.multiple_of(u * xt, xt), xt)], x_buf.at[slot], x_sem.at[slot])

    def o_store(u, j):
        return copy(o_buf.at[j], dw.at[j, pl.ds(pl.multiple_of(u * xt, xt), xt)], o_sem.at[j])

    def h_store(q):
        return copy(h_buf, hid.at[pl.ds(pl.multiple_of(q * qr, qr), qr)], h_sem)

    def go(*copies):
        for c in copies:
            c.start()

    def wait(*copies):
        for c in copies:
            c.wait()

    go(*dh_loads(0))
    go(*dh_loads(1))
    go(*gu_loads(0))
    go(*w_loads(0))
    go(*w_loads(1))

    barrier = pltpu.get_barrier_semaphore()
    for to in (n_d, n_x, n_y):
        pl.semaphore_signal(barrier, inc=1, device_id={"tp": to}, device_id_type=MESH)

    @pl.when(z > 0)
    def _():
        pl.semaphore_signal(barrier, inc=1, device_id={"tp": n_l}, device_id_type=MESH)

    @pl.when(z < 3)
    def _():
        pl.semaphore_signal(barrier, inc=1, device_id={"tp": n_r}, device_id_type=MESH)

    pl.semaphore_wait(barrier, jnp.where((z > 0) & (z < 3), 5, 4))

    first_bit, third_bit = (xx, y), (y, xx)
    first_to, third_to = (n_x, n_y), (n_y, n_x)
    hc = nc // 2

    def at_out(i, c, row, count, width=hc):
        r = lax.div(i, COLS) * qr + core * half + row
        k = lax.rem(i, COLS) * nc + c * hc
        return dx.at[pl.ds(pl.multiple_of(r, piece), count), pl.ds(pl.multiple_of(k, hc), width)]

    def slot_of(i, count):
        return lax.rem(i, count)

    def send_d(i):
        s, t = slot_of(i, N_TERM), slot_of(i, N_RD)
        src = term.at[s, pl.ds(pl.multiple_of((1 - core) * half, half), half)]
        return remote(src, r_d.at[t], d_snd.at[s], d_rcv.at[t], n_d)

    def send_1(i, c):
        s, t = slot_of(i, N_S1), slot_of(i, N_R1)
        src = s1.at[s, c, pl.ds(pl.multiple_of((1 - first_bit[c]) * quart, quart), quart)]
        return remote(src, r_1.at[t, c], s1_snd.at[s, c], s1_rcv.at[t, c], first_to[c])

    def send_z(i, c, right, row, count):
        s, t = slot_of(i, N_S2), slot_of(i, N_Z)
        src = s2.at[s, c, pl.ds(row * piece, count * piece)]
        buf, snd, rcv, to = (z_r, zr_snd, zr_rcv, n_r) if right else (z_l, zl_snd, zl_rcv, n_l)
        return remote(src, buf.at[t, c, pl.ds(0, count * piece)], snd.at[t, c], rcv.at[t, c], to)

    def own_piece(i, c):
        return s2.at[slot_of(i, N_S2), c, pl.ds(pl.multiple_of(z * piece, piece), piece)]

    def send_3(i, c):
        t = slot_of(i, N_R3)
        return remote(own_piece(i, c), r_3.at[t, c], s3_snd.at[t, c], s3_rcv.at[t, c], third_to[c])

    def keep_final(i, c):
        out = at_out(i, c, first_bit[c] * quart + z * piece, piece)
        return copy(own_piece(i, c), out, loc_sem.at[slot_of(i, N_SEM), c])

    def gather_z(i, c, right, first, count, fresh=False):
        ref = at_out(i, c, first_bit[c] * quart + first * piece, count * piece)
        snd, rcv, to = (gr_snd, gr_rcv, n_r) if right else (gl_snd, gl_rcv, n_l)
        s = slot_of(i, N_SEM)
        return remote(own_piece(i, c) if fresh else ref, ref, snd.at[s, c], rcv.at[s, c], to)

    def gather_1(i, c):
        ref, s = at_out(i, c, first_bit[c] * quart, quart), slot_of(i, N_SEM)
        return remote(ref, ref, a1_snd.at[s, c], a1_rcv.at[s, c], first_to[c])

    def gather_d(i):
        ref, s = at_out(i, 0, 0, half, nc), slot_of(i, N_SEM)
        return remote(ref, ref, ad_snd.at[s], ad_rcv.at[s], n_d)

    def on_line(*cases):
        for zz, body in cases:

            @pl.when(z == zz)
            def _(body=body):
                body()

    def both(body):
        for c in (0, 1):
            body(c)

    def add_piece(i, c, right, first, count):
        buf = z_r if right else z_l
        mine = s2.at[slot_of(i, N_S2), c, pl.ds(first * piece, count * piece)]
        add_rows(mine, mine, buf.at[slot_of(i, N_Z), c, pl.ds(0, count * piece)], count * piece, piece)

    def e12(i):
        gather_d(i).wait()
        both(lambda c: gather_1(i, c).wait_send())

        def middle(rights, lefts):
            def body():
                for c in (0, 1):
                    gather_z(i, c, True, *rights).wait_send()
                    gather_z(i, c, False, *lefts).wait_send()

            return body

        on_line((1, middle((0, 2), (1, 3))), (2, middle((0, 3), (2, 2))))

    def e11(i):
        both(lambda c: gather_1(i, c).wait_recv())
        gather_d(i).start()

    def e10(i):
        on_line(
            (3, lambda: both(lambda c: gather_z(i, c, True, 0, 3).wait_recv())),
            (0, lambda: both(lambda c: gather_z(i, c, False, 1, 3).wait_recv())),
        )
        both(lambda c: gather_1(i, c).start())

    def pass_on(i, right, got, gives):
        def body():
            for c in (0, 1):
                gather_z(i, c, right, *got).wait_recv()
                gather_z(i, c, right, *gives).start()

        return body

    def e9(i):
        on_line((2, pass_on(i, True, (0, 2), (0, 3))), (1, pass_on(i, False, (2, 2), (1, 3))))

    def e8(i):
        both(lambda c: keep_final(i, c).wait())
        on_line(
            (0, lambda: both(lambda c: gather_z(i, c, True, 0, 1, True).wait_send())),
            (1, pass_on(i, True, (0, 1), (0, 2))),
            (2, pass_on(i, False, (3, 1), (2, 2))),
            (3, lambda: both(lambda c: gather_z(i, c, False, 3, 1, True).wait_send())),
        )

    def e6(i):
        for c in (0, 1):
            send_3(i, c).wait()
            add_rows(own_piece(i, c), own_piece(i, c), r_3.at[slot_of(i, N_R3), c], piece, piece)

        def sent(rights, lefts):
            def body():
                for c in (0, 1):
                    if rights:
                        send_z(i, c, True, *rights).wait_send()
                    if lefts:
                        send_z(i, c, False, *lefts).wait_send()

            return body

        on_line(
            (0, sent((1, 3), None)),
            (1, sent((2, 2), (0, 1))),
            (2, sent((3, 1), (0, 2))),
            (3, sent(None, (0, 3))),
        )
        both(lambda c: keep_final(i, c).start())
        on_line(
            (0, lambda: both(lambda c: gather_z(i, c, True, 0, 1, True).start())),
            (3, lambda: both(lambda c: gather_z(i, c, False, 3, 1, True).start())),
        )

    def take(i, right, first, count, gives=None):
        def body():
            for c in (0, 1):
                send_z(i, c, right, first, count).wait_recv()
                add_piece(i, c, right, first, count)
                if gives:
                    send_z(i, c, right, *gives).start()

        return body

    def e5(i):
        on_line((3, take(i, True, 3, 1)), (0, take(i, False, 0, 1)))
        both(lambda c: send_3(i, c).start())

    def e4(i):
        on_line((2, take(i, True, 2, 2, (3, 1))), (1, take(i, False, 0, 2, (0, 1))))

    def e3(i):
        on_line((1, take(i, True, 1, 3, (2, 2))), (2, take(i, False, 0, 3, (0, 2))))

    def e2(i):
        for c in (0, 1):
            send_1(i, c).wait()
            kept = s1.at[slot_of(i, N_S1), c, pl.ds(pl.multiple_of(first_bit[c] * quart, quart), quart)]
            add_rows(s2.at[slot_of(i, N_S2), c], kept, r_1.at[slot_of(i, N_R1), c], quart, piece)
            on_line(
                (0, lambda c=c: send_z(i, c, True, 1, 3).start()),
                (3, lambda c=c: send_z(i, c, False, 0, 3).start()),
            )

    def e1(i):
        send_d(i).wait_recv()
        got = r_d.at[slot_of(i, N_RD)]
        for part in (0, 1):
            for c in (0, 1):
                b = first_bit[c] if part else 1 - first_bit[c]
                r = pl.ds(pl.multiple_of(b * quart, quart), quart)
                own = pl.ds(pl.multiple_of(core * half + b * quart, quart), quart)
                k = pl.ds(c * hc, hc)
                add_rows(
                    s1.at[slot_of(i, N_S1), c, r], term.at[slot_of(i, N_TERM), own, k], got.at[r, k], quart, piece
                )
        send_d(i).wait_send()
        both(lambda c: send_1(i, c).start())

    def e0(i):
        send_d(i).start()

    def activation(q):
        wait(*gu_loads(q))

        @pl.when(q > 0)
        def _():
            h_store(q - 1).wait()

        step = min(16, qr)

        def body(i, _):
            r = pl.ds(pl.multiple_of(i * step, step), step)
            to = pl.ds(pl.multiple_of(q * qr + i * step, step), step)
            g, u, dh = g_buf[r].astype(F32), u_buf[r].astype(F32), acc[r]
            sig = jax.nn.sigmoid(g)
            silu = g * sig
            h_buf[r] = (silu * u).astype(BF)
            d[to, pl.ds(ff, ff)] = (dh * silu).astype(BF)
            d[to, pl.ds(0, ff)] = (dh * u * (sig + silu * (1.0 - sig))).astype(BF)

        lax.fori_loop(0, qr // step, body, None)
        h_store(q).start()

        @pl.when(q + 1 < QUARTERS)
        def _():
            go(*gu_loads(q + 1))

    def dh_tile(m):
        q, j, slot = lax.div(m, KBLOCKS), lax.rem(m, KBLOCKS), lax.rem(m, 2)
        wait(*dh_loads(m))
        acc[...] = jnp.where(j == 0, 0.0, acc[...]) + dot(dy_buf[slot], wd_buf[slot], NT)

        @pl.when(m + 2 < DH)
        def _():
            go(*dh_loads(m + 2))

        @pl.when(j == KBLOCKS - 1)
        def _():
            activation(q)

    def dx_tile(k):
        slot = lax.rem(k, 2)
        r = pl.ds(pl.multiple_of(lax.div(k, COLS) * qr, qr), qr)
        wait(*w_loads(k))
        term[lax.rem(k, N_TERM)] = dot(d[r], w_buf[slot], NT).astype(BF)

        @pl.when(k + 2 < TILES)
        def _():
            go(*w_loads(k + 2))

    def dw_tile(u, j):
        slot = lax.rem(u, 2)

        @pl.when(j == 0)
        def _():
            x_load(u).wait()

        @pl.when(u > 0)
        def _():
            o_store(u - 1, j).wait()

        o_buf[j] = dot(x_buf[slot], d[:, pl.ds(pl.multiple_of(j * ff, ff), ff)], TN).astype(BF)
        o_store(u, j).start()

        @pl.when((j == 1) & (u + 2 < UNITS))
        def _():
            x_load(u + 2).start()

    steps = dict(e1=e1, e2=e2, e3=e3, e4=e4, e5=e5, e6=e6, e8=e8, e9=e9, e10=e10, e11=e11, e12=e12)

    def run_steps(n, half_trip):
        for name, event in reversed(steps.items()):
            lag, at_half = STEPS[name] // 2, STEPS[name] % 2
            if at_half == half_trip:
                i = n - lag

                @pl.when((i >= 0) & (i < TILES))
                def _(event=event, i=i):
                    event(i)

    def trip(t, _):
        n = t - KBLOCKS
        filler = n - LEAD

        @pl.when((n >= 0) & (n < TILES))
        def _():
            dx_tile(n)

        run_steps(n, 0)

        @pl.when((n >= 0) & (n < TILES))
        def _():
            e0(n)

        @pl.when((n < 0) | ((filler >= 0) & (filler < DH - KBLOCKS)))
        def _():
            dh_tile(jnp.where(n < 0, n + KBLOCKS, filler + KBLOCKS))

        @pl.when(n == 0)
        def _():
            go(x_load(0), x_load(1))

        w = filler - (DH - KBLOCKS)

        @pl.when((w >= 0) & (w < 2 * UNITS))
        def _():
            dw_tile(lax.div(w, 2), lax.rem(w, 2))

        run_steps(n, 1)

    lax.fori_loop(0, KBLOCKS + TRIPS, trip, None)
    h_store(QUARTERS - 1).wait()
    wait(o_store(UNITS - 1, 0), o_store(UNITS - 1, 1))


def main_call(x, dy, gate, up, w_gate, w_up, w_down):
    rows, cols = dy.shape
    ff = gate.shape[1]
    qr, nc, kb, xt = rows // QUARTERS, cols // COLS, cols // KBLOCKS, cols // UNITS
    half, quart, piece, hc = qr // 2, qr // 4, qr // 16, nc // 2
    dma = pltpu.SemaphoreType.DMA
    vmem = pltpu.VMEM
    anywhere = pl.BlockSpec(memory_space=pl.ANY)
    flops = 2 * rows * cols * ff * 5
    return pl.pallas_call(
        main_kernel,
        out_shape=(
            jax.ShapeDtypeStruct((rows, cols), BF),
            jax.ShapeDtypeStruct((rows, ff), BF),
            jax.ShapeDtypeStruct((2, cols, ff), BF),
        ),
        in_specs=[anywhere] * 7,
        out_specs=(anywhere,) * 3,
        scratch_shapes=[
            vmem((rows, 2 * ff), BF),
            vmem((2, nc, 2 * ff), BF),
            vmem((2, ff, kb), BF),
            vmem((2, qr, kb), BF),
            vmem((2, rows, xt), BF),
            vmem((qr, ff), BF),
            vmem((qr, ff), BF),
            vmem((qr, ff), F32),
            vmem((qr, ff), BF),
            vmem((2, xt, ff), BF),
            vmem((N_TERM, qr, nc), BF),
            vmem((N_RD, half, nc), BF),
            vmem((N_S1, 2, half, hc), BF),
            vmem((N_R1, 2, quart, hc), BF),
            vmem((N_S2, 2, quart, hc), BF),
            vmem((N_Z, 2, 3 * piece, hc), BF),
            vmem((N_Z, 2, 3 * piece, hc), BF),
            vmem((N_R3, 2, piece, hc), BF),
            dma((2, 2)), dma((2, 2)), dma((2,)), dma((2,)), dma, dma((2,)), dma((N_SEM, 2)),
            dma((N_TERM,)), dma((N_RD,)), dma((N_S1, 2)), dma((N_R1, 2)),
            dma((N_Z, 2)), dma((N_Z, 2)), dma((N_Z, 2)), dma((N_Z, 2)), dma((N_R3, 2)), dma((N_R3, 2)),
            dma((N_SEM, 2)), dma((N_SEM, 2)), dma((N_SEM, 2)), dma((N_SEM, 2)),
            dma((N_SEM, 2)), dma((N_SEM, 2)), dma((N_SEM,)), dma((N_SEM,)),
        ],
        compiler_params=pltpu.CompilerParams(
            collective_id=0, has_side_effects=True, vmem_limit_bytes=64_000_000
        ),
        cost_estimate=pl.CostEstimate(flops=flops, bytes_accessed=400 << 20, transcendentals=rows * ff),
        name="dx_reduce",
    )(x, dy, gate, up, w_gate, w_up, w_down)


def tail_kernel(hid, dy, dx_in, dw_in, dx, dw_gate, dw_up, dw_down, dx_buf, dw_buf, in_sem, out_sem):
    i, n = pl.program_id(0), pl.num_programs(0)
    slots, dx_rows, _ = dx_buf.shape
    dw_rows = dw_buf.shape[2]

    def loads(j):
        s = lax.rem(j, slots)
        a = pl.ds(pl.multiple_of(j * dx_rows, dx_rows), dx_rows)
        b = pl.ds(pl.multiple_of(j * dw_rows, dw_rows), dw_rows)
        return (
            pltpu.make_async_copy(dx_in.at[a], dx_buf.at[s], in_sem.at[s, 0]),
            pltpu.make_async_copy(dw_in.at[0, b], dw_buf.at[s, 0], in_sem.at[s, 1]),
            pltpu.make_async_copy(dw_in.at[1, b], dw_buf.at[s, 1], in_sem.at[s, 2]),
        )

    def stores(j):
        s = lax.rem(j, slots)
        a = pl.ds(pl.multiple_of(j * dx_rows, dx_rows), dx_rows)
        b = pl.ds(pl.multiple_of(j * dw_rows, dw_rows), dw_rows)
        return (
            pltpu.make_async_copy(dx_buf.at[s], dx.at[a], out_sem.at[s, 0]),
            pltpu.make_async_copy(dw_buf.at[s, 0], dw_gate.at[b], out_sem.at[s, 1]),
            pltpu.make_async_copy(dw_buf.at[s, 1], dw_up.at[b], out_sem.at[s, 2]),
        )

    ahead = slots // 2

    @pl.when(i == 0)
    def _():
        for j in range(ahead):
            for c in loads(j):
                c.start()

    @pl.when(i >= ahead)
    def _():
        for c in stores(i - ahead):
            c.wait()

    @pl.when(i + ahead < n)
    def _():
        for c in loads(i + ahead):
            c.start()

    for c in loads(i):
        c.wait()
    for c in stores(i):
        c.start()
    dw_down[...] = dot(hid[...], dy[...], TN).astype(BF)

    @pl.when(i == n - 1)
    def _():
        for j in range(ahead):
            for c in stores(n - ahead + j):
                c.wait()


def tail_call(hid, dy, dx, dw):
    rows, cols = dy.shape
    ff = hid.shape[1]
    n, slots = UNITS, 4
    spec, anywhere = pl.BlockSpec, pl.BlockSpec(memory_space=pl.ANY)
    return pl.pallas_call(
        tail_kernel,
        grid=(n,),
        out_shape=(
            jax.ShapeDtypeStruct((rows, cols), BF),
            jax.ShapeDtypeStruct((cols, ff), BF),
            jax.ShapeDtypeStruct((cols, ff), BF),
            jax.ShapeDtypeStruct((ff, cols), BF),
        ),
        in_specs=[
            spec((rows, ff), lambda i: (0, 0)),
            spec((rows, cols // n), lambda i: (0, i)),
            anywhere,
            anywhere,
        ],
        out_specs=(anywhere, anywhere, anywhere, spec((ff, cols // n), lambda i: (0, i))),
        scratch_shapes=[
            pltpu.VMEM((slots, rows // n, cols), BF),
            pltpu.VMEM((slots, 2, cols // n, ff), BF),
            pltpu.SemaphoreType.DMA((slots, 3)),
            pltpu.SemaphoreType.DMA((slots, 3)),
        ],
        compiler_params=pltpu.CompilerParams(vmem_limit_bytes=60_000_000),
        cost_estimate=pl.CostEstimate(
            flops=2 * rows * cols * ff, bytes_accessed=180 << 20, transcendentals=0
        ),
        name="dw_down_and_copies",
    )(hid, dy, dx, dw)


def solution(mesh):
    def step(x, dy, gate, up, w_gate, w_up, w_down):
        dx, hid, dw = main_call(x, dy, gate, up, w_gate, w_up, w_down)
        return tail_call(hid, dy, dx, dw)

    tokens, columns, rows = P("dp", None), P(None, "tp"), P("tp", None)
    return jax.shard_map(
        step,
        mesh=mesh,
        in_specs=(tokens, tokens, P("dp", "tp"), P("dp", "tp"), columns, columns, rows),
        out_specs=(tokens, P("dp", "tp"), P("dp", "tp"), P(("dp", "tp"), None)),
        check_vma=False,
    )
```

```python
import jax
import jax.numpy as jnp
from jax import lax
from jax.experimental import pallas as pl
from jax.experimental.pallas import tpu as pltpu
from jax.sharding import PartitionSpec as P

BF, F32 = jnp.bfloat16, jnp.float32
MESH = pl.DeviceIdType.MESH
NT = (((1,), (1,)), ((), ()))
TN = (((0,), (0,)), ((), ()))

QUARTERS = 4
COLS = 8
TILES = QUARTERS * COLS
KBLOCKS = 4
UNITS = 16
DH = QUARTERS * KBLOCKS
LEAD = 4
STEPS = dict(
    e1=3, e2=7, e3=9, e4=11, e5=13, e6=16, e8=18, e9=22, e10=30, e11=34, e12=38,
)
FILLERS = DH - KBLOCKS + 2 * UNITS
TRIPS = max(LEAD + FILLERS, TILES + STEPS["e12"] // 2 + 1)
N_TERM, N_RD, N_S1, N_R1, N_S2, N_Z, N_R3, N_SEM = 2, 4, 4, 8, 8, 8, 8, 16


def dot(a, b, dims):
    return lax.dot_general(a, b, dims, preferred_element_type=F32)


def add_rows(dst, a, b, rows, block):
    def body(i, _):
        r = pl.ds(pl.multiple_of(i * block, block), block)
        dst[r] = (a[r].astype(F32) + b[r].astype(F32)).astype(BF)

    lax.fori_loop(0, rows // block, body, None)


def main_kernel(
    x, dy, gate, up, w_gate, w_up, w_down, dx, hid, dw,
    d, w_buf, wd_buf, dy_buf, x_buf, g_buf, u_buf, acc, h_buf, o_buf,
    term, r_d, s1, r_1, s2, z_r, z_l, r_3,
    w_sem, dh_sem, x_sem, gu_sem, h_sem, o_sem, loc_sem,
    d_snd, d_rcv, s1_snd, s1_rcv, zr_snd, zr_rcv, zl_snd, zl_rcv, s3_snd, s3_rcv,
    gr_snd, gr_rcv, gl_snd, gl_rcv, a1_snd, a1_rcv, ad_snd, ad_rcv,
):
    rows, cols = dy.shape
    ff = gate.shape[1]
    qr, nc, kb, xt = rows // QUARTERS, cols // COLS, cols // KBLOCKS, cols // UNITS
    half, quart, piece = qr // 2, qr // 4, qr // 16

    me = lax.axis_index("tp")
    core, z = lax.rem(me, 2), lax.rem(lax.div(me, 2), 4)
    y, xx = lax.rem(lax.div(me, 8), 2), lax.div(me, 16)
    n_d = me + 1 - 2 * core
    n_x, n_y = me + 16 * (1 - 2 * xx), me + 8 * (1 - 2 * y)
    n_r, n_l = me + 2, me - 2

    def copy(src, dst, sem):
        return pltpu.make_async_copy(src, dst, sem)

    def remote(src, dst, snd, rcv, to):
        return pltpu.make_async_remote_copy(
            src_ref=src, dst_ref=dst, send_sem=snd, recv_sem=rcv,
            device_id={"tp": to}, device_id_type=MESH,
        )

    def dh_loads(m):
        q, j, slot = lax.div(m, KBLOCKS), lax.rem(m, KBLOCKS), lax.rem(m, 2)
        k = pl.ds(pl.multiple_of(j * kb, kb), kb)
        r = pl.ds(pl.multiple_of(q * qr, qr), qr)
        return (
            copy(dy.at[r, k], dy_buf.at[slot], dh_sem.at[0, slot]),
            copy(w_down.at[:, k], wd_buf.at[slot], dh_sem.at[1, slot]),
        )

    def gu_loads(q):
        r = pl.ds(pl.multiple_of(q * qr, qr), qr)
        return copy(gate.at[r], g_buf, gu_sem.at[0]), copy(up.at[r], u_buf, gu_sem.at[1])

    def w_loads(k):
        slot = lax.rem(k, 2)
        r = pl.ds(pl.multiple_of(lax.rem(k, COLS) * nc, nc), nc)
        return (
            copy(w_gate.at[r], w_buf.at[slot, :, pl.ds(0, ff)], w_sem.at[0, slot]),
            copy(w_up.at[r], w_buf.at[slot, :, pl.ds(ff, ff)], w_sem.at[1, slot]),
        )

    def x_load(u):
        slot = lax.rem(u, 2)
        return copy(x.at[:, pl.ds(pl.multiple_of(u * xt, xt), xt)], x_buf.at[slot], x_sem.at[slot])

    def o_store(u, j):
        return copy(o_buf.at[j], dw.at[j, pl.ds(pl.multiple_of(u * xt, xt), xt)], o_sem.at[j])

    def h_store(q):
        return copy(h_buf, hid.at[pl.ds(pl.multiple_of(q * qr, qr), qr)], h_sem)

    def go(*copies):
        for c in copies:
            c.start()

    def wait(*copies):
        for c in copies:
            c.wait()

    go(*dh_loads(0))
    go(*dh_loads(1))
    go(*gu_loads(0))

    barrier = pltpu.get_barrier_semaphore()
    for to in (n_d, n_x, n_y):
        pl.semaphore_signal(barrier, inc=1, device_id={"tp": to}, device_id_type=MESH)

    @pl.when(z > 0)
    def _():
        pl.semaphore_signal(barrier, inc=1, device_id={"tp": n_l}, device_id_type=MESH)

    @pl.when(z < 3)
    def _():
        pl.semaphore_signal(barrier, inc=1, device_id={"tp": n_r}, device_id_type=MESH)

    pl.semaphore_wait(barrier, jnp.where((z > 0) & (z < 3), 5, 4))

    first_bit, third_bit = (xx, y), (y, xx)
    first_to, third_to = (n_x, n_y), (n_y, n_x)
    hc = nc // 2

    def at_out(i, c, row, count, width=hc):
        r = lax.div(i, COLS) * qr + core * half + row
        k = lax.rem(i, COLS) * nc + c * hc
        return dx.at[pl.ds(pl.multiple_of(r, piece), count), pl.ds(pl.multiple_of(k, hc), width)]

    def slot_of(i, count):
        return lax.rem(i, count)

    def send_d(i):
        s, t = slot_of(i, N_TERM), slot_of(i, N_RD)
        src = term.at[s, pl.ds(pl.multiple_of((1 - core) * half, half), half)]
        return remote(src, r_d.at[t], d_snd.at[s], d_rcv.at[t], n_d)

    def send_1(i, c):
        s, t = slot_of(i, N_S1), slot_of(i, N_R1)
        src = s1.at[s, c, pl.ds(pl.multiple_of((1 - first_bit[c]) * quart, quart), quart)]
        return remote(src, r_1.at[t, c], s1_snd.at[s, c], s1_rcv.at[t, c], first_to[c])

    def send_z(i, c, right, row, count):
        s, t = slot_of(i, N_S2), slot_of(i, N_Z)
        src = s2.at[s, c, pl.ds(row * piece, count * piece)]
        buf, snd, rcv, to = (z_r, zr_snd, zr_rcv, n_r) if right else (z_l, zl_snd, zl_rcv, n_l)
        return remote(src, buf.at[t, c, pl.ds(0, count * piece)], snd.at[t, c], rcv.at[t, c], to)

    def own_piece(i, c):
        return s2.at[slot_of(i, N_S2), c, pl.ds(pl.multiple_of(z * piece, piece), piece)]

    def send_3(i, c):
        t = slot_of(i, N_R3)
        return remote(own_piece(i, c), r_3.at[t, c], s3_snd.at[t, c], s3_rcv.at[t, c], third_to[c])

    def keep_final(i, c):
        out = at_out(i, c, first_bit[c] * quart + z * piece, piece)
        return copy(own_piece(i, c), out, loc_sem.at[slot_of(i, N_SEM), c])

    def gather_z(i, c, right, first, count, fresh=False):
        ref = at_out(i, c, first_bit[c] * quart + first * piece, count * piece)
        snd, rcv, to = (gr_snd, gr_rcv, n_r) if right else (gl_snd, gl_rcv, n_l)
        s = slot_of(i, N_SEM)
        return remote(own_piece(i, c) if fresh else ref, ref, snd.at[s, c], rcv.at[s, c], to)

    def gather_1(i, c):
        ref, s = at_out(i, c, first_bit[c] * quart, quart), slot_of(i, N_SEM)
        return remote(ref, ref, a1_snd.at[s, c], a1_rcv.at[s, c], first_to[c])

    def gather_d(i):
        ref, s = at_out(i, 0, 0, half, nc), slot_of(i, N_SEM)
        return remote(ref, ref, ad_snd.at[s], ad_rcv.at[s], n_d)

    def on_line(*cases):
        for zz, body in cases:

            @pl.when(z == zz)
            def _(body=body):
                body()

    def both(body):
        for c in (0, 1):
            body(c)

    def add_piece(i, c, right, first, count):
        buf = z_r if right else z_l
        mine = s2.at[slot_of(i, N_S2), c, pl.ds(first * piece, count * piece)]
        add_rows(mine, mine, buf.at[slot_of(i, N_Z), c, pl.ds(0, count * piece)], count * piece, piece)

    def e12(i):
        gather_d(i).wait()
        both(lambda c: gather_1(i, c).wait_send())

        def middle(rights, lefts):
            def body():
                for c in (0, 1):
                    gather_z(i, c, True, *rights).wait_send()
                    gather_z(i, c, False, *lefts).wait_send()

            return body

        on_line((1, middle((0, 2), (1, 3))), (2, middle((0, 3), (2, 2))))

    def e11(i):
        both(lambda c: gather_1(i, c).wait_recv())
        gather_d(i).start()

    def e10(i):
        on_line(
            (3, lambda: both(lambda c: gather_z(i, c, True, 0, 3).wait_recv())),
            (0, lambda: both(lambda c: gather_z(i, c, False, 1, 3).wait_recv())),
        )
        both(lambda c: gather_1(i, c).start())

    def pass_on(i, right, got, gives):
        def body():
            for c in (0, 1):
                gather_z(i, c, right, *got).wait_recv()
                gather_z(i, c, right, *gives).start()

        return body

    def e9(i):
        on_line((2, pass_on(i, True, (0, 2), (0, 3))), (1, pass_on(i, False, (2, 2), (1, 3))))

    def e8(i):
        both(lambda c: keep_final(i, c).wait())
        on_line(
            (0, lambda: both(lambda c: gather_z(i, c, True, 0, 1, True).wait_send())),
            (1, pass_on(i, True, (0, 1), (0, 2))),
            (2, pass_on(i, False, (3, 1), (2, 2))),
            (3, lambda: both(lambda c: gather_z(i, c, False, 3, 1, True).wait_send())),
        )

    def e6(i):
        for c in (0, 1):
            send_3(i, c).wait()
            add_rows(own_piece(i, c), own_piece(i, c), r_3.at[slot_of(i, N_R3), c], piece, piece)

        def sent(rights, lefts):
            def body():
                for c in (0, 1):
                    if rights:
                        send_z(i, c, True, *rights).wait_send()
                    if lefts:
                        send_z(i, c, False, *lefts).wait_send()

            return body

        on_line(
            (0, sent((1, 3), None)),
            (1, sent((2, 2), (0, 1))),
            (2, sent((3, 1), (0, 2))),
            (3, sent(None, (0, 3))),
        )
        both(lambda c: keep_final(i, c).start())
        on_line(
            (0, lambda: both(lambda c: gather_z(i, c, True, 0, 1, True).start())),
            (3, lambda: both(lambda c: gather_z(i, c, False, 3, 1, True).start())),
        )

    def take(i, right, first, count, gives=None):
        def body():
            for c in (0, 1):
                send_z(i, c, right, first, count).wait_recv()
                add_piece(i, c, right, first, count)
                if gives:
                    send_z(i, c, right, *gives).start()

        return body

    def e5(i):
        on_line((3, take(i, True, 3, 1)), (0, take(i, False, 0, 1)))
        both(lambda c: send_3(i, c).start())

    def e4(i):
        on_line((2, take(i, True, 2, 2, (3, 1))), (1, take(i, False, 0, 2, (0, 1))))

    def e3(i):
        on_line((1, take(i, True, 1, 3, (2, 2))), (2, take(i, False, 0, 3, (0, 2))))

    def e2(i):
        for c in (0, 1):
            send_1(i, c).wait()
            kept = s1.at[slot_of(i, N_S1), c, pl.ds(pl.multiple_of(first_bit[c] * quart, quart), quart)]
            add_rows(s2.at[slot_of(i, N_S2), c], kept, r_1.at[slot_of(i, N_R1), c], quart, piece)
            on_line(
                (0, lambda c=c: send_z(i, c, True, 1, 3).start()),
                (3, lambda c=c: send_z(i, c, False, 0, 3).start()),
            )

    def e1(i):
        send_d(i).wait_recv()
        got = r_d.at[slot_of(i, N_RD)]
        for part in (0, 1):
            for c in (0, 1):
                b = first_bit[c] if part else 1 - first_bit[c]
                r = pl.ds(pl.multiple_of(b * quart, quart), quart)
                own = pl.ds(pl.multiple_of(core * half + b * quart, quart), quart)
                k = pl.ds(c * hc, hc)
                add_rows(
                    s1.at[slot_of(i, N_S1), c, r], term.at[slot_of(i, N_TERM), own, k], got.at[r, k], quart, piece
                )
        send_d(i).wait_send()
        both(lambda c: send_1(i, c).start())

    def e0(i):
        send_d(i).start()

    def activation(q):
        wait(*gu_loads(q))

        @pl.when(q > 0)
        def _():
            h_store(q - 1).wait()

        step = min(16, qr)

        def body(i, _):
            r = pl.ds(pl.multiple_of(i * step, step), step)
            to = pl.ds(pl.multiple_of(q * qr + i * step, step), step)
            g, u, dh = g_buf[r].astype(F32), u_buf[r].astype(F32), acc[r]
            sig = jax.nn.sigmoid(g)
            silu = g * sig
            h_buf[r] = (silu * u).astype(BF)
            d[to, pl.ds(ff, ff)] = (dh * silu).astype(BF)
            d[to, pl.ds(0, ff)] = (dh * u * (sig + silu * (1.0 - sig))).astype(BF)

        lax.fori_loop(0, qr // step, body, None)
        h_store(q).start()

        @pl.when(q + 1 < QUARTERS)
        def _():
            go(*gu_loads(q + 1))

    def dh_tile(m):
        q, j, slot = lax.div(m, KBLOCKS), lax.rem(m, KBLOCKS), lax.rem(m, 2)
        wait(*dh_loads(m))
        acc[...] = jnp.where(j == 0, 0.0, acc[...]) + dot(dy_buf[slot], wd_buf[slot], NT)

        @pl.when(m + 2 < DH)
        def _():
            go(*dh_loads(m + 2))

        @pl.when((m == 1) | (m == KBLOCKS - 1))
        def _():
            go(*w_loads(lax.div(m, 2)))

        @pl.when(j == KBLOCKS - 1)
        def _():
            activation(q)

    def dx_tile(k):
        slot = lax.rem(k, 2)
        r = pl.ds(pl.multiple_of(lax.div(k, COLS) * qr, qr), qr)
        wait(*w_loads(k))
        term[lax.rem(k, N_TERM)] = dot(d[r], w_buf[slot], NT).astype(BF)

        @pl.when(k + 2 < TILES)
        def _():
            go(*w_loads(k + 2))

    def dw_tile(u, j):
        slot = lax.rem(u, 2)

        @pl.when(j == 0)
        def _():
            x_load(u).wait()

        @pl.when(u > 0)
        def _():
            o_store(u - 1, j).wait()

        o_buf[j] = dot(x_buf[slot], d[:, pl.ds(pl.multiple_of(j * ff, ff), ff)], TN).astype(BF)
        o_store(u, j).start()

        @pl.when((j == 1) & (u + 2 < UNITS))
        def _():
            x_load(u + 2).start()

    steps = dict(e1=e1, e2=e2, e3=e3, e4=e4, e5=e5, e6=e6, e8=e8, e9=e9, e10=e10, e11=e11, e12=e12)

    def run_steps(n, half_trip):
        for name, event in reversed(steps.items()):
            lag, at_half = STEPS[name] // 2, STEPS[name] % 2
            if at_half == half_trip:
                i = n - lag

                @pl.when((i >= 0) & (i < TILES))
                def _(event=event, i=i):
                    event(i)

    def trip(t, _):
        n = t - KBLOCKS
        filler = n - LEAD

        @pl.when((n >= 0) & (n < TILES))
        def _():
            dx_tile(n)

        run_steps(n, 0)

        @pl.when((n >= 0) & (n < TILES))
        def _():
            e0(n)

        @pl.when((n < 0) | ((filler >= 0) & (filler < DH - KBLOCKS)))
        def _():
            dh_tile(jnp.where(n < 0, n + KBLOCKS, filler + KBLOCKS))

        @pl.when(n == 0)
        def _():
            go(x_load(0), x_load(1))

        w = filler - (DH - KBLOCKS)

        @pl.when((w >= 0) & (w < 2 * UNITS))
        def _():
            dw_tile(lax.div(w, 2), lax.rem(w, 2))

        run_steps(n, 1)

    lax.fori_loop(0, KBLOCKS + TRIPS, trip, None)
    h_store(QUARTERS - 1).wait()
    wait(o_store(UNITS - 1, 0), o_store(UNITS - 1, 1))


def main_call(x, dy, gate, up, w_gate, w_up, w_down):
    rows, cols = dy.shape
    ff = gate.shape[1]
    qr, nc, kb, xt = rows // QUARTERS, cols // COLS, cols // KBLOCKS, cols // UNITS
    half, quart, piece, hc = qr // 2, qr // 4, qr // 16, nc // 2
    dma = pltpu.SemaphoreType.DMA
    vmem = pltpu.VMEM
    anywhere = pl.BlockSpec(memory_space=pl.ANY)
    flops = 2 * rows * cols * ff * 5
    return pl.pallas_call(
        main_kernel,
        out_shape=(
            jax.ShapeDtypeStruct((rows, cols), BF),
            jax.ShapeDtypeStruct((rows, ff), BF),
            jax.ShapeDtypeStruct((2, cols, ff), BF),
        ),
        in_specs=[anywhere] * 7,
        out_specs=(anywhere,) * 3,
        scratch_shapes=[
            vmem((rows, 2 * ff), BF),
            vmem((2, nc, 2 * ff), BF),
            vmem((2, ff, kb), BF),
            vmem((2, qr, kb), BF),
            vmem((2, rows, xt), BF),
            vmem((qr, ff), BF),
            vmem((qr, ff), BF),
            vmem((qr, ff), F32),
            vmem((qr, ff), BF),
            vmem((2, xt, ff), BF),
            vmem((N_TERM, qr, nc), BF),
            vmem((N_RD, half, nc), BF),
            vmem((N_S1, 2, half, hc), BF),
            vmem((N_R1, 2, quart, hc), BF),
            vmem((N_S2, 2, quart, hc), BF),
            vmem((N_Z, 2, 3 * piece, hc), BF),
            vmem((N_Z, 2, 3 * piece, hc), BF),
            vmem((N_R3, 2, piece, hc), BF),
            dma((2, 2)), dma((2, 2)), dma((2,)), dma((2,)), dma, dma((2,)), dma((N_SEM, 2)),
            dma((N_TERM,)), dma((N_RD,)), dma((N_S1, 2)), dma((N_R1, 2)),
            dma((N_Z, 2)), dma((N_Z, 2)), dma((N_Z, 2)), dma((N_Z, 2)), dma((N_R3, 2)), dma((N_R3, 2)),
            dma((N_SEM, 2)), dma((N_SEM, 2)), dma((N_SEM, 2)), dma((N_SEM, 2)),
            dma((N_SEM, 2)), dma((N_SEM, 2)), dma((N_SEM,)), dma((N_SEM,)),
        ],
        compiler_params=pltpu.CompilerParams(
            collective_id=0, has_side_effects=True, vmem_limit_bytes=64_000_000
        ),
        cost_estimate=pl.CostEstimate(flops=flops, bytes_accessed=400 << 20, transcendentals=rows * ff),
        name="dx_reduce",
    )(x, dy, gate, up, w_gate, w_up, w_down)


def tail_kernel(
    hid, dy, dx_in, dw_in, dx, dw_gate, dw_up, dw_down, dx_buf, dw_buf, hid_buf, in_sem, out_sem, hid_sem
):
    i, n = pl.program_id(0), pl.num_programs(0)
    slots, dx_rows, _ = dx_buf.shape
    dw_rows = dw_buf.shape[2]

    def loads(j):
        s = lax.rem(j, slots)
        a = pl.ds(pl.multiple_of(j * dx_rows, dx_rows), dx_rows)
        b = pl.ds(pl.multiple_of(j * dw_rows, dw_rows), dw_rows)
        return (
            pltpu.make_async_copy(dx_in.at[a], dx_buf.at[s], in_sem.at[s, 0]),
            pltpu.make_async_copy(dw_in.at[0, b], dw_buf.at[s, 0], in_sem.at[s, 1]),
            pltpu.make_async_copy(dw_in.at[1, b], dw_buf.at[s, 1], in_sem.at[s, 2]),
        )

    def stores(j):
        s = lax.rem(j, slots)
        a = pl.ds(pl.multiple_of(j * dx_rows, dx_rows), dx_rows)
        b = pl.ds(pl.multiple_of(j * dw_rows, dw_rows), dw_rows)
        return (
            pltpu.make_async_copy(dx_buf.at[s], dx.at[a], out_sem.at[s, 0]),
            pltpu.make_async_copy(dw_buf.at[s, 0], dw_gate.at[b], out_sem.at[s, 1]),
            pltpu.make_async_copy(dw_buf.at[s, 1], dw_up.at[b], out_sem.at[s, 2]),
        )

    ahead = slots // 2

    @pl.when(i == 0)
    def _():
        pltpu.make_async_copy(hid, hid_buf, hid_sem).start()
        for j in range(ahead):
            for c in loads(j):
                c.start()

    @pl.when(i >= ahead)
    def _():
        for c in stores(i - ahead):
            c.wait()

    @pl.when(i + ahead < n)
    def _():
        for c in loads(i + ahead):
            c.start()

    for c in loads(i):
        c.wait()
    for c in stores(i):
        c.start()

    @pl.when(i == 0)
    def _():
        pltpu.make_async_copy(hid, hid_buf, hid_sem).wait()

    dw_down[...] = dot(hid_buf[...], dy[...], TN).astype(BF)

    @pl.when(i == n - 1)
    def _():
        for j in range(ahead):
            for c in stores(n - ahead + j):
                c.wait()


def tail_call(hid, dy, dx, dw):
    rows, cols = dy.shape
    ff = hid.shape[1]
    n, slots = UNITS, 4
    spec, anywhere = pl.BlockSpec, pl.BlockSpec(memory_space=pl.ANY)
    return pl.pallas_call(
        tail_kernel,
        grid=(n,),
        out_shape=(
            jax.ShapeDtypeStruct((rows, cols), BF),
            jax.ShapeDtypeStruct((cols, ff), BF),
            jax.ShapeDtypeStruct((cols, ff), BF),
            jax.ShapeDtypeStruct((ff, cols), BF),
        ),
        in_specs=[
            anywhere,
            spec((rows, cols // n), lambda i: (0, i)),
            anywhere,
            anywhere,
        ],
        out_specs=(anywhere, anywhere, anywhere, spec((ff, cols // n), lambda i: (0, i))),
        scratch_shapes=[
            pltpu.VMEM((slots, rows // n, cols), BF),
            pltpu.VMEM((slots, 2, cols // n, ff), BF),
            pltpu.VMEM((rows, ff), BF),
            pltpu.SemaphoreType.DMA((slots, 3)),
            pltpu.SemaphoreType.DMA((slots, 3)),
            pltpu.SemaphoreType.DMA,
        ],
        compiler_params=pltpu.CompilerParams(vmem_limit_bytes=60_000_000),
        cost_estimate=pl.CostEstimate(
            flops=2 * rows * cols * ff, bytes_accessed=180 << 20, transcendentals=0
        ),
        name="dw_down_and_copies",
    )(hid, dy, dx, dw)


def solution(mesh):
    def step(x, dy, gate, up, w_gate, w_up, w_down):
        dx, hid, dw = main_call(x, dy, gate, up, w_gate, w_up, w_down)
        return tail_call(hid, dy, dx, dw)

    tokens, columns, rows = P("dp", None), P(None, "tp"), P("tp", None)
    return jax.shard_map(
        step,
        mesh=mesh,
        in_specs=(tokens, tokens, P("dp", "tp"), P("dp", "tp"), columns, columns, rows),
        out_specs=(tokens, P("dp", "tp"), P("dp", "tp"), P(("dp", "tp"), None)),
        check_vma=False,
    )
```
